256 devices in a mesh: atom: 32 (over x_lo, z, core), freq: 8 (over x_hi, y).
Axes of the slice: x: 4 (x_hi: 2, x_lo: 2; x = x_hi * 2 + x_lo), y: 4, z: 8, core: 2. Of those that a mesh axis runs over, the one named last changes fastest.
Arguments:
- feats: bfloat16 [65536, 256], P('atom'), may hold values from -6 to 6
- positions: float32 [3, 65536], P(None, 'atom'), may hold values from 0 to 2
- phases: bfloat16 [2, 65536, 1024], P(None, 'atom', 'freq')
- filt: float32 [1024, 256], P('freq'), may hold values from 0.3 to 3
- w_value: bfloat16 [256, 256], replicated, may hold values from -0.375 to 0.375
- neighbour_tiles: int32 [512, 8], P(('atom', 'freq')), may hold values from 0 to 511, as said below
- neighbour_count: int32 [512], P(('atom', 'freq')), may hold values from 1 to 8, as said below
Outputs:
- updated: bfloat16 [65536, 256], P(('atom', 'freq'))
The draws below stay inside these ranges and needn't reach their ends.
Inputs may be any that keep to these rules, and one draw needn't show every extreme that they name: `neighbour_tiles`: a tile's entries are distinct tiles of its own block of 16 tiles (tiles b * 16 to (b + 1) * 16 - 1) or of the block just before or after it, counted around the ends. `neighbour_count`: some tile has 8.
All inputs are finite; a program needn't handle non-finite values.
Results may differ from the reference program's by a relative error of at most 0.0095.
Values may be sent and summed in bfloat16 or wider, within the bound.
A program may use at most 64 MiB of HBM per device.

```python
import math
import jax
import jax.numpy as jnp
from jax import lax

C = 256
K = 1024
TILE = 128
NB = 8
ATOMS = 65536
TILES_DEV = 16
TILES = 512


def draw_phases(key, part):
    angle = jax.random.uniform(key, (ATOMS, K), jnp.float32, -math.pi, math.pi)
    return jnp.stack([jnp.cos(angle), jnp.sin(angle)]).astype(jnp.bfloat16)


def draw_neighbour_tiles(key, part):
    keys = jax.random.split(jax.random.fold_in(key, 11), TILES)
    picks = jax.vmap(lambda single: jax.random.permutation(single, 3 * TILES_DEV)[:NB])(keys).astype(jnp.int32)
    blocks = TILES // TILES_DEV
    home = (jnp.arange(TILES, dtype=jnp.int32) // TILES_DEV)[:, None]
    target = (home + picks // TILES_DEV - 1 + blocks) % blocks
    return (target * TILES_DEV + picks % TILES_DEV).astype(jnp.int32)


def draw_neighbour_count(key, part):
    first, second, third = jax.random.split(jax.random.fold_in(key, 23), 3)
    blocks = TILES // TILES_DEV
    ceiling = jax.random.randint(first, (blocks, 1), NB // 2, NB + 1)
    counts = jax.random.randint(second, (blocks, TILES_DEV), 1, ceiling + 1).reshape(TILES)
    chosen = jax.random.randint(third, (), 0, TILES)
    return jnp.where(jnp.arange(TILES, dtype=jnp.int32) == chosen, NB, counts).astype(jnp.int32)


def block_levels(stream_key, shape, cuts, low, largest):
    loudness = 1.0
    for position, blocks in cuts:
        heights = jax.random.uniform(jax.random.fold_in(jax.random.fold_in(stream_key, 6), position), (blocks,), jnp.float32, low / len(cuts), largest / len(cuts))
        loudness = loudness * jnp.repeat(jnp.exp(heights), shape[position] // blocks).reshape((-1,) + (1,) * (len(shape) - 1 - position))
    return loudness


def gaussian(stream_key, shape, spread, reach, cuts=(), held_as=jnp.bfloat16):
    drawn = jax.random.normal(stream_key, shape, jnp.float32) * spread
    if len(cuts) > 0:
        drawn = block_levels(stream_key, shape, cuts, -0.22, 0.18) * drawn
    return jnp.clip(drawn, min=-reach, max=reach).astype(held_as)


def setup_inputs(seed: int = 0) -> dict:
    streams_of = jax.random.split(jax.random.key(seed), 8)
    return {
        "feats": gaussian(streams_of[0], (ATOMS, C), 1.0, 6.0, ((0, 32),)),
        "positions": jnp.clip(2.0 * jax.random.uniform(streams_of[1], (3, ATOMS), jnp.float32) ** block_levels(streams_of[1], (3, ATOMS), ((1, 32),), -0.2, 0.2), 0.0, 2.0),
        "phases": draw_phases(jax.random.fold_in(streams_of[7], 71), 0),
        "filt": jnp.clip(jnp.exp(math.log(3.0) - 2.3025851 * jax.random.uniform(streams_of[3], (K, C), jnp.float32) ** block_levels(streams_of[3], (K, C), ((0, 8),), -0.2, 0.2)), 0.3, 3.0),
        "w_value": gaussian(streams_of[4], (C, C), C ** -0.5, 0.375),
        "neighbour_tiles": draw_neighbour_tiles(jax.random.fold_in(streams_of[7], 71), 0),
        "neighbour_count": draw_neighbour_count(jax.random.fold_in(streams_of[7], 71), 0),
    }


def reference(feats, positions, phases, filt, w_value, neighbour_tiles, neighbour_count):
    struct = lax.dot_general(phases, feats, (((1,), (0,)), ((), ())), preferred_element_type=jnp.float32)
    scale = 1.0 / math.sqrt(ATOMS * K)
    filtered = (filt[None] * struct * scale).astype(jnp.bfloat16)
    long_msg = jnp.dot(phases[0], filtered[0], preferred_element_type=jnp.float32) + jnp.dot(phases[1], filtered[1], preferred_element_type=jnp.float32)
    values = jnp.dot(feats, w_value, preferred_element_type=jnp.float32).astype(jnp.bfloat16)
    blocks = TILES // TILES_DEV
    v_tiles = values.reshape(TILES, TILE, C)
    p_tiles = positions.reshape(3, TILES, TILE)
    own_all = positions.reshape(3, blocks, TILES_DEV, TILE).transpose(1, 0, 2, 3)

    def one_block(items):
        ids, count, own = items
        near_v = v_tiles[ids].astype(jnp.float32)
        near_p = p_tiles[:, ids]
        dist = jnp.zeros((TILES_DEV, TILE, NB, TILE), jnp.float32)
        for axis_c in range(3):
            diff = own[axis_c][:, :, None, None] - near_p[axis_c][:, None, :, :]
            dist = dist + diff * diff
        live = (jnp.arange(NB, dtype=jnp.int32)[None, :] < count[:, None]).astype(jnp.float32)
        weight = lax.optimization_barrier((jnp.exp(-dist) * live[:, None, :, None]).astype(jnp.bfloat16)).astype(jnp.float32)
        return jnp.einsum('tinj,tnjc->tic', weight, near_v, precision=lax.Precision.HIGHEST)
    short = lax.map(one_block, (neighbour_tiles.reshape(blocks, TILES_DEV, NB), neighbour_count.reshape(blocks, TILES_DEV), own_all))
    short_msg = short.reshape(ATOMS, C) / math.sqrt(TILE)
    return (feats.astype(jnp.float32) + long_msg + short_msg).astype(jnp.bfloat16)
```

```python
import functools
import math

import jax
import jax.numpy as jnp
from jax import lax
from jax.experimental import pallas as pl
from jax.experimental.pallas import tpu as pltpu
from jax.sharding import PartitionSpec as P

MESH = pl.DeviceIdType.MESH
TILE = 128
CHUNKS = 4
FIRST = 448
FAR = 1e30

F32 = jnp.float32
BF16 = jnp.bfloat16


def dot(a, b):
    return jnp.dot(a, b, preferred_element_type=F32)


def kernel(
    scale,
    feats_hbm,
    pos_hbm,
    phases_hbm,
    filt_hbm,
    w_hbm,
    tiles_smem,
    count_smem,
    out_ref,
    feats,
    pos,
    ph,
    ph2,
    filt,
    w,
    values,
    weight,
    req_pos,
    req_ids,
    in_pos,
    in_ids,
    columns,
    short,
    sh_send,
    sh_recv,
    rs_send,
    rs_recv,
    gat,
    l_own,
    l_send,
    l_recv,
    in_sem,
    rs_ssem,
    rs_rsem,
    ph_ssem,
    ph_rsem,
    rq_ssem,
    rq_rsem,
    sh_ssem,
    sh_rsem,
    ag_ssem,
    ag_rsem,
    sw_ssem,
    sw_rsem,
    l_ssem,
    l_rsem,
):
    a = lax.axis_index("atom")
    f = lax.axis_index("freq")
    core = lax.rem(a, 2)
    row = a // 2
    x_lo = row // 8
    z = lax.rem(row, 8)
    x_hi = f // 4
    y = lax.rem(f, 4)
    other = (1 - x_hi) * 4 + y

    def remote(src, dst, ssem, rsem, to):
        return pltpu.make_async_remote_copy(
            src_ref=src, dst_ref=dst, send_sem=ssem, recv_sem=rsem, device_id=to, device_id_type=MESH
        )

    step = 2048 // CHUNKS
    loads = [
        pltpu.make_async_copy(pos_hbm, pos, in_sem.at[0]),
        pltpu.make_async_copy(filt_hbm, filt, in_sem.at[1]),
        pltpu.make_async_copy(w_hbm, w, in_sem.at[2]),
    ]
    chunk_loads = []
    for i in range(CHUNKS):
        rows = pl.ds(i * step, step)
        trio = [
            pltpu.make_async_copy(phases_hbm.at[0, rows], ph.at[rows, pl.ds(0, 128)], in_sem.at[3 + 3 * i]),
            pltpu.make_async_copy(phases_hbm.at[1, rows], ph.at[rows, pl.ds(128, 128)], in_sem.at[4 + 3 * i]),
            pltpu.make_async_copy(feats_hbm.at[rows], feats.at[rows], in_sem.at[5 + 3 * i]),
        ]
        for c in trio:
            c.start()
        chunk_loads.append(trio)
    for c in loads:
        c.start()

    barrier = pltpu.get_barrier_semaphore()

    def greet(j, carry):
        pl.semaphore_signal(barrier, inc=1, device_id=(lax.rem(a + j, 32), f), device_id_type=MESH)
        return carry

    lax.fori_loop(1, 32, greet, 0)
    pl.semaphore_signal(barrier, inc=1, device_id=(a, other), device_id_type=MESH)
    for j in range(1, 4):
        pl.semaphore_signal(barrier, inc=1, device_id=(a, x_hi * 4 + lax.rem(y + j, 4)), device_id_type=MESH)

    total = None
    for i in range(CHUNKS):
        for c in chunk_loads[i]:
            c.wait()
        rows = pl.ds(i * step, step)
        part = lax.dot_general(
            ph[rows, :], feats[rows, :], (((0,), (0,)), ((), ())), preferred_element_type=F32
        )
        total = part if total is None else total + part
    for h in range(2):
        rs_send[h * 16 : (h + 1) * 16] = total[:, h * 128 : (h + 1) * 128].astype(BF16).reshape(16, 16, 128)

    loads[0].wait()
    req_pos[...] = jnp.zeros_like(req_pos)
    req_pos[0:3, :] = pos[:, pl.ds(pl.multiple_of(f * 256, 256), 256)]
    for t in range(2):
        for n in range(8):
            tile = jnp.where(n < count_smem[t], tiles_smem[t, n], -1)
            req_ids[t * 8 + n : t * 8 + n + 1, :] = jnp.full((1, 128), tile, jnp.int32)

    pl.semaphore_wait(barrier, 35)

    def send_part(j, carry):
        to = lax.rem(a + j, 32)
        remote(
            rs_send.at[lax.rem(to, 2) * 16 + to // 2], rs_recv.at[j], rs_ssem, rs_rsem, (to, f)
        ).start()
        return carry

    lax.fori_loop(1, 32, send_part, 0)
    before, after = lax.rem(a + 31, 32), lax.rem(a + 1, 32)
    asks = []
    for i, to in enumerate((before, after)):
        asks.append(remote(req_pos, in_pos.at[i], rq_ssem.at[2 * i], rq_rsem.at[2 * i], (to, f)))
        asks.append(remote(req_ids, in_ids.at[i], rq_ssem.at[2 * i + 1], rq_rsem.at[2 * i + 1], (to, f)))
    for c in asks:
        c.start()
    half = (1 - x_hi) * 1024
    early = remote(
        ph.at[pl.ds(half, FIRST)], ph2.at[pl.ds(0, FIRST)], ph_ssem.at[0], ph_rsem.at[0], (a, other)
    )
    late = remote(
        ph.at[pl.ds(half + FIRST, 1024 - FIRST)],
        ph2.at[pl.ds(FIRST, 1024 - FIRST)],
        ph_ssem.at[1],
        ph_rsem.at[1],
        (a, other),
    )
    early.start()

    loads[2].wait()
    for i in range(CHUNKS):
        rows = pl.ds(i * step, step)
        values[rows, :] = dot(feats[rows, :], w[...]).astype(BF16)

    def query(pos_ref, ids_ref):
        flipped = pos_ref[...].T
        for c in range(3):
            columns[c] = jnp.broadcast_to(flipped[:, c : c + 1], (256, 128))

        def tile(s, carry):
            lanes = pl.ds(pl.multiple_of(s * TILE, TILE), TILE)
            mine = a * 16 + s
            theirs = pos[:, lanes]
            for t in range(2):
                rows = pl.ds(t * TILE, TILE)
                live = jnp.max((ids_ref[t * 8 : (t + 1) * 8, :] == mine).astype(F32), axis=0, keepdims=True)
                dist = (1.0 - live) * FAR
                for c in range(3):
                    diff = columns[c, rows, :] - theirs[c : c + 1, :]
                    dist = dist + diff * diff
                weight[rows, lanes] = jnp.exp(-dist).astype(BF16)
            return carry

        lax.fori_loop(0, 16, tile, 0)
        return dot(weight[...], values[...])

    short[...] = query(req_pos, req_ids)

    parts = rs_recv.at[pl.ds(1, 31)]
    pltpu.make_async_copy(parts, parts, rs_rsem).wait()
    share = rs_send[core * 16 + row].astype(F32)
    share = share + jnp.sum(rs_recv[1:32].astype(F32), axis=0)
    loads[1].wait()
    k_rows = pl.ds(pl.multiple_of(lax.rem(row, 8) * 16, 16), 16)
    filt_share = jnp.where(core == 0, filt[k_rows, 0:128], filt[k_rows, 128:256])
    gat[core, row] = (filt_share * share * scale).astype(BF16)

    def send_share(k, carry):
        to = lax.rem((x_hi * 2 + x_lo) * 8 + z + k, 32)
        to_x, to_z = to // 8, lax.rem(to, 8)
        to_hi, to_lo = to_x // 2, lax.rem(to_x, 2)
        slot = lax.rem(to_hi + x_hi, 2) * 16 + row
        remote(
            gat.at[core, row],
            gat.at[core, slot],
            ag_ssem,
            ag_rsem,
            ((to_lo * 8 + to_z) * 2 + core, to_hi * 4 + y),
        ).start()
        return carry

    lax.fori_loop(1, 32, send_share, 0)
    late.start()

    answers = []
    for i, to in enumerate((before, after)):
        asks[2 * i].wait_recv()
        asks[2 * i + 1].wait_recv()
        sh_send[i] = query(in_pos.at[i], in_ids.at[i]).astype(BF16)
        answer = remote(
            sh_send.at[i], sh_recv.at[i], sh_ssem.at[i], sh_rsem.at[i], ((after, before)[i], f)
        )
        answer.start()
        answers.append(answer)

    shares = rs_recv.at[pl.ds(1, 31)]
    pltpu.make_async_copy(shares, shares, ag_rsem).wait()
    swap = remote(gat.at[core], gat.at[core], sw_ssem, sw_rsem, (row * 2 + 1 - core, f))
    swap.start()
    early.wait_recv()
    late.wait_recv()
    swap.wait_recv()

    mine = jnp.concatenate([gat[0, 0:16].reshape(256, 128), gat[1, 0:16].reshape(256, 128)], axis=1)
    twin = jnp.concatenate([gat[0, 16:32].reshape(256, 128), gat[1, 16:32].reshape(256, 128)], axis=1)

    def message(to):
        here = pl.ds(pl.multiple_of((x_hi * 4 + to) * 256, 256), 256)
        there = pl.ds(pl.multiple_of(to * 256, 256), 256)
        return dot(ph[here, :], mine) + dot(ph2[there, :], twin)

    sends = []
    for j in (2, 1, 3):
        to = lax.rem(y + j, 4)
        l_send[j - 1] = message(to).astype(BF16)
        c = remote(
            l_send.at[j - 1], l_recv.at[j - 1], l_ssem.at[j - 1], l_rsem.at[j - 1], (a, x_hi * 4 + to)
        )
        c.start()
        sends.append(c)
    l_own[...] = message(y)

    for c in answers:
        c.wait_recv()
    near = short[...] + sh_recv[0].astype(F32) + sh_recv[1].astype(F32)
    own = feats[pl.ds(pl.multiple_of(f * 256, 256), 256), :].astype(F32)
    l_own[...] = l_own[...] + near * (1.0 / math.sqrt(TILE)) + own
    for c in sends:
        c.wait_recv()
    far = l_recv[0].astype(F32) + l_recv[1].astype(F32) + l_recv[2].astype(F32)
    out_ref[...] = (l_own[...] + far).astype(BF16)

    pltpu.make_async_copy(parts, parts, rs_ssem).wait()
    pltpu.make_async_copy(parts, parts, ag_ssem).wait()
    for c in asks + answers + sends + [early, late, swap]:
        c.wait_send()


def shards(feats, positions, phases, filt, w_value, neighbour_tiles, neighbour_count):
    n_atom = lax.axis_size("atom")
    n_freq = lax.axis_size("freq")
    scale = 1.0 / math.sqrt(feats.shape[0] * n_atom * phases.shape[2] * n_freq)
    any_space = pl.BlockSpec(memory_space=pl.ANY)
    smem = pl.BlockSpec(memory_space=pltpu.SMEM)
    vmem, dma = pltpu.VMEM, pltpu.SemaphoreType.DMA
    return pl.pallas_call(
        functools.partial(kernel, scale),
        out_shape=jax.ShapeDtypeStruct((256, 256), BF16),
        in_specs=[any_space] * 5 + [smem] * 2,
        out_specs=pl.BlockSpec(memory_space=pltpu.VMEM),
        scratch_shapes=[
            vmem((2048, 256), BF16),
            vmem((3, 2048), F32),
            vmem((2048, 256), BF16),
            vmem((1024, 256), BF16),
            vmem((128, 256), F32),
            vmem((256, 256), BF16),
            vmem((2048, 256), BF16),
            vmem((256, 2048), BF16),
            vmem((8, 256), F32),
            vmem((16, 128), jnp.int32),
            vmem((2, 8, 256), F32),
            vmem((2, 16, 128), jnp.int32),
            vmem((3, 256, 128), F32),
            vmem((256, 256), F32),
            vmem((2, 256, 256), BF16),
            vmem((2, 256, 256), BF16),
            vmem((32, 16, 128), BF16),
            vmem((32, 16, 128), BF16),
            vmem((2, 32, 16, 128), BF16),
            vmem((256, 256), F32),
            vmem((3, 256, 256), BF16),
            vmem((3, 256, 256), BF16),
            dma((3 + 3 * CHUNKS,)),
            dma,
            dma,
            dma((2,)),
            dma((2,)),
            dma((4,)),
            dma((4,)),
            dma((2,)),
            dma((2,)),
            dma,
            dma,
            dma,
            dma,
            dma((3,)),
            dma((3,)),
        ],
        compiler_params=pltpu.CompilerParams(
            collective_id=0, has_side_effects=True, vmem_limit_bytes=66_000_000
        ),
    )(feats, positions, phases, filt, w_value, neighbour_tiles, neighbour_count)


def solution(mesh):
    in_specs = (
        P("atom", None),
        P(None, "atom"),
        P(None, "atom", "freq"),
        P("freq", None),
        P(),
        P(("atom", "freq"), None),
        P(("atom", "freq")),
    )
    out_specs = P(("atom", "freq"), None)
    return jax.shard_map(shards, mesh=mesh, in_specs=in_specs, out_specs=out_specs, check_vma=False)
```

```python
import functools
import math

import jax
import jax.numpy as jnp
from jax import lax
from jax.experimental import pallas as pl
from jax.experimental.pallas import tpu as pltpu
from jax.sharding import PartitionSpec as P

MESH = pl.DeviceIdType.MESH
TILE = 128
CHUNKS = 2
FAR = 1e30

F32 = jnp.float32
BF16 = jnp.bfloat16


def dot(a, b):
    return jnp.dot(a, b, preferred_element_type=F32)


def kernel(
    scale,
    feats_hbm,
    pos_hbm,
    phases_hbm,
    filt_hbm,
    w_hbm,
    tiles_smem,
    count_smem,
    out_ref,
    feats,
    pos,
    ph,
    lent,
    filt,
    w,
    values,
    weight,
    req_pos,
    req_ids,
    in_pos,
    in_ids,
    columns,
    short,
    sh_send,
    sh_recv,
    rs_send,
    rs_recv,
    gat,
    l_own,
    l_send,
    l_recv,
    in_sem,
    rs_ssem,
    rs_rsem,
    ph_ssem,
    ph_rsem,
    rq_ssem,
    rq_rsem,
    sh_ssem,
    sh_rsem,
    az_ssem,
    az_rsem,
    ap_ssem,
    ap_rsem,
    sw_ssem,
    sw_rsem,
    l_ssem,
    l_rsem,
):
    a = lax.axis_index("atom")
    f = lax.axis_index("freq")
    core = lax.rem(a, 2)
    row = a // 2
    x_lo = row // 8
    z = lax.rem(row, 8)
    x_hi = f // 4
    y = lax.rem(f, 4)
    other = (1 - x_hi) * 4 + y

    def remote(src, dst, ssem, rsem, to):
        return pltpu.make_async_remote_copy(
            src_ref=src, dst_ref=dst, send_sem=ssem, recv_sem=rsem, device_id=to, device_id_type=MESH
        )

    step = 2048 // CHUNKS
    loads = [
        pltpu.make_async_copy(pos_hbm, pos, in_sem.at[0]),
        pltpu.make_async_copy(filt_hbm, filt, in_sem.at[1]),
        pltpu.make_async_copy(w_hbm, w, in_sem.at[2]),
    ]
    chunk_loads = []
    for i in range(CHUNKS):
        rows = pl.ds(i * step, step)
        trio = [
            pltpu.make_async_copy(phases_hbm.at[0, rows], ph.at[rows, pl.ds(0, 128)], in_sem.at[3 + 3 * i]),
            pltpu.make_async_copy(phases_hbm.at[1, rows], ph.at[rows, pl.ds(128, 128)], in_sem.at[4 + 3 * i]),
            pltpu.make_async_copy(feats_hbm.at[rows], feats.at[rows], in_sem.at[5 + 3 * i]),
        ]
        for c in trio:
            c.start()
        chunk_loads.append(trio)
    for c in loads:
        c.start()

    barrier = pltpu.get_barrier_semaphore()

    def greet(j, carry):
        pl.semaphore_signal(barrier, inc=1, device_id=(lax.rem(a + j, 32), f), device_id_type=MESH)
        return carry

    lax.fori_loop(1, 32, greet, 0)
    pl.semaphore_signal(barrier, inc=1, device_id=(a, other), device_id_type=MESH)
    for j in range(1, 4):
        pl.semaphore_signal(barrier, inc=1, device_id=(a, x_hi * 4 + lax.rem(y + j, 4)), device_id_type=MESH)

    total = None
    for i in range(CHUNKS):
        for c in chunk_loads[i]:
            c.wait()
        rows = pl.ds(i * step, step)
        part = lax.dot_general(
            ph[rows, :], feats[rows, :], (((0,), (0,)), ((), ())), preferred_element_type=F32
        )
        total = part if total is None else total + part
    for h in range(2):
        rs_send[h * 16 : (h + 1) * 16] = total[:, h * 128 : (h + 1) * 128].astype(BF16).reshape(16, 16, 128)

    loads[0].wait()
    req_pos[...] = jnp.zeros_like(req_pos)
    req_pos[0:3, :] = pos[:, pl.ds(pl.multiple_of(f * 256, 256), 256)]
    for t in range(2):
        for n in range(8):
            tile = jnp.where(n < count_smem[t], tiles_smem[t, n], -1)
            req_ids[t * 8 + n : t * 8 + n + 1, :] = jnp.full((1, 128), tile, jnp.int32)

    pl.semaphore_wait(barrier, 35)

    def send_part(j, carry):
        to = lax.rem(a + j, 32)
        remote(
            rs_send.at[lax.rem(to, 2) * 16 + to // 2], rs_recv.at[j], rs_ssem, rs_rsem, (to, f)
        ).start()
        return carry

    lax.fori_loop(1, 32, send_part, 0)
    before, after = lax.rem(a + 31, 32), lax.rem(a + 1, 32)
    asks = []
    for i, to in enumerate((before, after)):
        asks.append(remote(req_pos, in_pos.at[i], rq_ssem.at[2 * i], rq_rsem.at[2 * i], (to, f)))
        asks.append(remote(req_ids, in_ids.at[i], rq_ssem.at[2 * i + 1], rq_rsem.at[2 * i + 1], (to, f)))
    for c in asks:
        c.start()

    def lend(j, hi):
        to = lax.rem(y + j, 4)
        rows = pl.ds(pl.multiple_of((lax.rem(x_hi + hi, 2) * 4 + to) * 256, 256), 256)
        i = (j - 1) * 2 + hi
        return remote(
            ph.at[rows], lent.at[j - 1, hi], ph_ssem.at[i], ph_rsem.at[i], (a, x_hi * 4 + to)
        )

    loans = {(j, hi): lend(j, hi) for hi in (1, 0) for j in (1, 3, 2)}
    for key in ((1, 1), (3, 1), (2, 1), (1, 0), (3, 0)):
        loans[key].start()

    loads[2].wait()
    for i in range(CHUNKS):
        rows = pl.ds(i * step, step)
        values[rows, :] = dot(feats[rows, :], w[...]).astype(BF16)

    def query(pos_ref, ids_ref):
        flipped = pos_ref[...].T
        for c in range(3):
            columns[c] = jnp.broadcast_to(flipped[:, c : c + 1], (256, 128))

        def tile(s, carry):
            lanes = pl.ds(pl.multiple_of(s * TILE, TILE), TILE)
            mine = a * 16 + s
            theirs = pos[:, lanes]
            for t in range(2):
                rows = pl.ds(t * TILE, TILE)
                live = jnp.max((ids_ref[t * 8 : (t + 1) * 8, :] == mine).astype(F32), axis=0, keepdims=True)
                dist = (1.0 - live) * FAR
                for c in range(3):
                    diff = columns[c, rows, :] - theirs[c : c + 1, :]
                    dist = dist + diff * diff
                weight[rows, lanes] = jnp.exp(-dist).astype(BF16)
            return carry

        lax.fori_loop(0, 16, tile, 0)
        return dot(weight[...], values[...])

    short[...] = query(req_pos, req_ids)

    parts = rs_recv.at[pl.ds(1, 31)]
    pltpu.make_async_copy(parts, parts, rs_rsem).wait()
    share = rs_send[core * 16 + row].astype(F32)
    share = share + jnp.sum(rs_recv[1:32].astype(F32), axis=0)
    loads[1].wait()
    k_rows = pl.ds(pl.multiple_of(lax.rem(row, 8) * 16, 16), 16)
    filt_share = jnp.where(core == 0, filt[k_rows, 0:128], filt[k_rows, 128:256])
    gat[core, 0, x_lo, z] = (filt_share * share * scale).astype(BF16)

    along_z = []
    for j in (4, 3, 5, 2, 6, 1, 7):
        to = (x_lo * 8 + lax.rem(z + j, 8)) * 2 + core
        mine = gat.at[core, 0, x_lo, z]
        along_z.append(remote(mine, mine, az_ssem, az_rsem, (to, f)))
        along_z[-1].start()

    answers = []

    def answer(i, to):
        asks[2 * i].wait_recv()
        asks[2 * i + 1].wait_recv()
        sh_send[i] = query(in_pos.at[i], in_ids.at[i]).astype(BF16)
        answers.append(remote(sh_send.at[i], sh_recv.at[i], sh_ssem.at[i], sh_rsem.at[i], (to, f)))
        answers[-1].start()

    answer(0, after)
    seven = gat.at[0, 0, 0, pl.ds(0, 7)]
    pltpu.make_async_copy(seven, seven, az_rsem).wait()
    plane = []
    for j, flip in ((2, 1), (2, 0), (1, 1), (3, 1), (1, 0), (3, 0), (0, 1)):
        to = ((lax.rem(x_lo + flip, 2) * 8 + z) * 2 + core, x_hi * 4 + lax.rem(y + j, 4))
        plane.append(
            remote(gat.at[core, 0, x_lo], gat.at[core, (4 - j) % 4, x_lo], ap_ssem, ap_rsem, to)
        )
        plane[-1].start()
    loans[2, 0].start()
    seven_rows = feats.at[pl.ds(0, 7 * 64)]
    answer(1, before)
    pltpu.make_async_copy(seven_rows, seven_rows, ap_rsem).wait()
    swap = remote(gat.at[core], gat.at[core], sw_ssem, sw_rsem, (row * 2 + 1 - core, f))
    swap.start()

    def message(hi, filtered):
        rows = pl.ds(pl.multiple_of((lax.rem(x_hi + hi, 2) * 4 + y) * 256, 256), 256)
        out = dot(ph[rows, :], filtered(0))
        for j in range(1, 4):
            out = out + dot(lent[j - 1, hi], filtered(4 - j))
        return out

    def half(h):
        return lambda j: gat[h, j].reshape(256, 128)

    def whole(j):
        return jnp.concatenate([gat[0, j].reshape(256, 128), gat[1, j].reshape(256, 128)], axis=1)

    for j in (1, 3, 2):
        loans[j, 1].wait_recv()
    sends = []
    for i, h in enumerate((core, 1 - core)):
        if i == 1:
            swap.wait_recv()
        l_send[h] = message(1, half(h)).astype(BF16)
        sends.append(remote(l_send.at[h], l_recv.at[h], l_ssem.at[i], l_rsem.at[i], (a, other)))
        sends[-1].start()
    for j in (1, 3, 2):
        loans[j, 0].wait_recv()
    l_own[...] = message(0, whole)

    for c in answers:
        c.wait_recv()
    near = short[...] + sh_recv[0].astype(F32) + sh_recv[1].astype(F32)
    own = feats[pl.ds(pl.multiple_of(f * 256, 256), 256), :].astype(F32)
    l_own[...] = l_own[...] + near * (1.0 / math.sqrt(TILE)) + own
    for c in sends:
        c.wait_recv()
    far = jnp.concatenate([l_recv[0].astype(F32), l_recv[1].astype(F32)], axis=1)
    out_ref[...] = (l_own[...] + far).astype(BF16)

    pltpu.make_async_copy(parts, parts, rs_ssem).wait()
    pltpu.make_async_copy(seven, seven, az_ssem).wait()
    pltpu.make_async_copy(seven_rows, seven_rows, ap_ssem).wait()
    for c in asks + answers + sends + [swap] + list(loans.values()):
        c.wait_send()


def shards(feats, positions, phases, filt, w_value, neighbour_tiles, neighbour_count):
    n_atom = lax.axis_size("atom")
    n_freq = lax.axis_size("freq")
    scale = 1.0 / math.sqrt(feats.shape[0] * n_atom * phases.shape[2] * n_freq)
    any_space = pl.BlockSpec(memory_space=pl.ANY)
    smem = pl.BlockSpec(memory_space=pltpu.SMEM)
    vmem, dma = pltpu.VMEM, pltpu.SemaphoreType.DMA
    return pl.pallas_call(
        functools.partial(kernel, scale),
        out_shape=jax.ShapeDtypeStruct((256, 256), BF16),
        in_specs=[any_space] * 5 + [smem] * 2,
        out_specs=pl.BlockSpec(memory_space=pltpu.VMEM),
        scratch_shapes=[
            vmem((2048, 256), BF16),
            vmem((3, 2048), F32),
            vmem((2048, 256), BF16),
            vmem((3, 2, 256, 256), BF16),
            vmem((128, 256), F32),
            vmem((256, 256), BF16),
            vmem((2048, 256), BF16),
            vmem((256, 2048), BF16),
            vmem((8, 256), F32),
            vmem((16, 128), jnp.int32),
            vmem((2, 8, 256), F32),
            vmem((2, 16, 128), jnp.int32),
            vmem((3, 256, 128), F32),
            vmem((256, 256), F32),
            vmem((2, 256, 256), BF16),
            vmem((2, 256, 256), BF16),
            vmem((32, 16, 128), BF16),
            vmem((32, 16, 128), BF16),
            vmem((2, 4, 2, 8, 16, 128), BF16),
            vmem((256, 256), F32),
            vmem((2, 256, 128), BF16),
            vmem((2, 256, 128), BF16),
            dma((3 + 3 * CHUNKS,)),
            dma,
            dma,
            dma((6,)),
            dma((6,)),
            dma((4,)),
            dma((4,)),
            dma((2,)),
            dma((2,)),
            dma,
            dma,
            dma,
            dma,
            dma,
            dma,
            dma((2,)),
            dma((2,)),
        ],
        compiler_params=pltpu.CompilerParams(
            collective_id=0, has_side_effects=True, vmem_limit_bytes=66_000_000
        ),
    )(feats, positions, phases, filt, w_value, neighbour_tiles, neighbour_count)


def solution(mesh):
    in_specs = (
        P("atom", None),
        P(None, "atom"),
        P(None, "atom", "freq"),
        P("freq", None),
        P(),
        P(("atom", "freq"), None),
        P(("atom", "freq")),
    )
    out_specs = P(("atom", "freq"), None)
    return jax.shard_map(shards, mesh=mesh, in_specs=in_specs, out_specs=out_specs, check_vma=False)
```

```python
import functools
import math

import jax
import jax.numpy as jnp
from jax import lax
from jax.experimental import pallas as pl
from jax.experimental.pallas import tpu as pltpu
from jax.sharding import PartitionSpec as P

MESH = pl.DeviceIdType.MESH
TILE = 128
CHUNKS = 2
FAR = 1e30
ATOM_PEERS = [(i, j, k) for j in (4, 3, 5, 2, 6, 1, 7, 0) for i in (1, 0) for k in (1, 0) if i + j + k > 0]

F32 = jnp.float32
BF16 = jnp.bfloat16


def dot(a, b):
    return jnp.dot(a, b, preferred_element_type=F32)


def kernel(
    scale,
    feats_hbm,
    pos_hbm,
    phases_hbm,
    filt_hbm,
    w_hbm,
    tiles_hbm,
    count_hbm,
    out_ref,
    tiles_smem,
    count_smem,
    feats,
    pos,
    ph,
    lent,
    filt,
    w,
    values,
    weight,
    req_pos,
    req_ids,
    in_pos,
    in_ids,
    columns,
    short,
    sh_send,
    sh_recv,
    rs_send,
    rs_recv,
    gat,
    l_own,
    l_send,
    l_recv,
    in_sem,
    rs_ssem,
    rs_rsem,
    ph_ssem,
    ph_rsem,
    rq_ssem,
    rq_rsem,
    sh_ssem,
    sh_rsem,
    az_ssem,
    az_rsem,
    ap_ssem,
    ap_rsem,
    sw_ssem,
    sw_rsem,
    l_ssem,
    l_rsem,
):
    a = lax.axis_index("atom")
    f = lax.axis_index("freq")
    core = lax.rem(a, 2)
    row = a // 2
    x_lo = row // 8
    z = lax.rem(row, 8)
    x_hi = f // 4
    y = lax.rem(f, 4)
    other = (1 - x_hi) * 4 + y

    def remote(src, dst, ssem, rsem, to):
        return pltpu.make_async_remote_copy(
            src_ref=src, dst_ref=dst, send_sem=ssem, recv_sem=rsem, device_id=to, device_id_type=MESH
        )

    z_at = [lax.rem(z + j, 8) * 2 for j in range(8)]
    x_at = [x_lo * 16, (1 - x_lo) * 16]
    core_at = [core, 1 - core]

    def block_at(d):
        return x_at[d[0]] + z_at[d[1]] + core_at[d[2]]

    barrier = pltpu.get_barrier_semaphore()

    def greet(to):
        pl.semaphore_signal(barrier, inc=1, device_id=to, device_id_type=MESH)

    for d in ATOM_PEERS:
        greet((block_at(d), f))
    for j in (2, 1, 3):
        greet((a, x_hi * 4 + lax.rem(y + j, 4)))
    greet((a, other))

    step = 2048 // CHUNKS
    loads = [
        pltpu.make_async_copy(pos_hbm, pos, in_sem.at[0]),
        pltpu.make_async_copy(filt_hbm, filt, in_sem.at[1]),
        pltpu.make_async_copy(w_hbm, w, in_sem.at[2]),
        pltpu.make_async_copy(tiles_hbm, tiles_smem, in_sem.at[3]),
        pltpu.make_async_copy(count_hbm, count_smem, in_sem.at[4]),
    ]
    chunk_loads = []
    for i in range(CHUNKS):
        rows = pl.ds(i * step, step)
        trio = [
            pltpu.make_async_copy(phases_hbm.at[0, rows], ph.at[rows, pl.ds(0, 128)], in_sem.at[5 + 3 * i]),
            pltpu.make_async_copy(phases_hbm.at[1, rows], ph.at[rows, pl.ds(128, 128)], in_sem.at[6 + 3 * i]),
            pltpu.make_async_copy(feats_hbm.at[rows], feats.at[rows], in_sem.at[7 + 3 * i]),
        ]
        for c in trio:
            c.start()
        chunk_loads.append(trio)
    for c in loads:
        c.start()

    total = None
    for i in range(CHUNKS):
        for c in chunk_loads[i]:
            c.wait()
        rows = pl.ds(i * step, step)
        part = lax.dot_general(
            ph[rows, :], feats[rows, :], (((0,), (0,)), ((), ())), preferred_element_type=F32
        )
        total = part if total is None else total + part
    for h in range(2):
        rs_send[h * 16 : (h + 1) * 16] = total[:, h * 128 : (h + 1) * 128].astype(BF16).reshape(16, 16, 128)

    loads[0].wait()
    loads[3].wait()
    loads[4].wait()
    req_pos[...] = jnp.zeros_like(req_pos)
    req_pos[0:3, :] = pos[:, pl.ds(pl.multiple_of(f * 256, 256), 256)]
    for t in range(2):
        for n in range(8):
            tile = jnp.where(n < count_smem[t], tiles_smem[t, n], -1)
            req_ids[t * 8 + n : t * 8 + n + 1, :] = jnp.full((1, 128), tile, jnp.int32)

    pl.semaphore_wait(barrier, 35)

    for i, d in enumerate(ATOM_PEERS):
        to = block_at(d)
        share_of = core_at[d[2]] * 16 + (x_at[d[0]] + z_at[d[1]]) // 2
        remote(rs_send.at[share_of], rs_recv.at[i + 1], rs_ssem, rs_rsem, (to, f)).start()
    before, after = lax.rem(a + 31, 32), lax.rem(a + 1, 32)
    asks = []
    for i, to in enumerate((before, after)):
        asks.append(remote(req_pos, in_pos.at[i], rq_ssem.at[2 * i], rq_rsem.at[2 * i], (to, f)))
        asks.append(remote(req_ids, in_ids.at[i], rq_ssem.at[2 * i + 1], rq_rsem.at[2 * i + 1], (to, f)))
    for c in asks:
        c.start()

    def lend(j, hi):
        to = lax.rem(y + j, 4)
        rows = pl.ds(pl.multiple_of((lax.rem(x_hi + hi, 2) * 4 + to) * 256, 256), 256)
        i = (j - 1) * 2 + hi
        return remote(
            ph.at[rows], lent.at[j - 1, hi], ph_ssem.at[i], ph_rsem.at[i], (a, x_hi * 4 + to)
        )

    loans = {(j, hi): lend(j, hi) for hi in (1, 0) for j in (1, 3, 2)}
    for key in ((1, 1), (3, 1), (2, 1), (1, 0), (3, 0)):
        loans[key].start()

    loads[2].wait()
    for i in range(CHUNKS):
        rows = pl.ds(i * step, step)
        values[rows, :] = dot(feats[rows, :], w[...]).astype(BF16)

    def query(pos_ref, ids_ref):
        flipped = pos_ref[...].T
        for c in range(3):
            columns[c] = jnp.broadcast_to(flipped[:, c : c + 1], (256, 128))

        def tile(s, carry):
            lanes = pl.ds(pl.multiple_of(s * TILE, TILE), TILE)
            mine = a * 16 + s
            theirs = pos[:, lanes]
            for t in range(2):
                rows = pl.ds(t * TILE, TILE)
                live = jnp.max((ids_ref[t * 8 : (t + 1) * 8, :] == mine).astype(F32), axis=0, keepdims=True)
                dist = (1.0 - live) * FAR
                for c in range(3):
                    diff = columns[c, rows, :] - theirs[c : c + 1, :]
                    dist = dist + diff * diff
                weight[rows, lanes] = jnp.exp(-dist).astype(BF16)
            return carry

        lax.fori_loop(0, 16, tile, 0)
        return dot(weight[...], values[...])

    short[...] = query(req_pos, req_ids)

    parts = rs_recv.at[pl.ds(1, 31)]
    pltpu.make_async_copy(parts, parts, rs_rsem).wait()
    share = rs_send[core * 16 + row].astype(F32)
    share = share + jnp.sum(rs_recv[1:32].astype(F32), axis=0)
    loads[1].wait()
    k_rows = pl.ds(pl.multiple_of(lax.rem(row, 8) * 16, 16), 16)
    filt_share = jnp.where(core == 0, filt[k_rows, 0:128], filt[k_rows, 128:256])
    gat[core, 0, x_lo, z] = (filt_share * share * scale).astype(BF16)

    along_z = []
    for j in (4, 3, 5, 2, 6, 1, 7):
        to = (x_lo * 8 + lax.rem(z + j, 8)) * 2 + core
        mine = gat.at[core, 0, x_lo, z]
        along_z.append(remote(mine, mine, az_ssem, az_rsem, (to, f)))
        along_z[-1].start()

    answers = []

    def answer(i, to):
        asks[2 * i].wait_recv()
        asks[2 * i + 1].wait_recv()
        sh_send[i] = query(in_pos.at[i], in_ids.at[i]).astype(BF16)
        answers.append(remote(sh_send.at[i], sh_recv.at[i], sh_ssem.at[i], sh_rsem.at[i], (to, f)))
        answers[-1].start()

    answer(0, after)
    seven = gat.at[0, 0, 0, pl.ds(0, 7)]
    pltpu.make_async_copy(seven, seven, az_rsem).wait()
    plane = []
    for j, flip in ((2, 1), (2, 0), (1, 1), (3, 1), (1, 0), (3, 0), (0, 1)):
        to = ((lax.rem(x_lo + flip, 2) * 8 + z) * 2 + core, x_hi * 4 + lax.rem(y + j, 4))
        plane.append(
            remote(gat.at[core, 0, x_lo], gat.at[core, (4 - j) % 4, x_lo], ap_ssem, ap_rsem, to)
        )
        plane[-1].start()
    loans[2, 0].start()
    seven_rows = feats.at[pl.ds(0, 7 * 64)]
    answer(1, before)
    pltpu.make_async_copy(seven_rows, seven_rows, ap_rsem).wait()
    swap = remote(gat.at[core], gat.at[core], sw_ssem, sw_rsem, (row * 2 + 1 - core, f))
    swap.start()

    def message(hi, filtered):
        rows = pl.ds(pl.multiple_of((lax.rem(x_hi + hi, 2) * 4 + y) * 256, 256), 256)
        out = dot(ph[rows, :], filtered(0))
        for j in range(1, 4):
            out = out + dot(lent[j - 1, hi], filtered(4 - j))
        return out

    def half(h):
        return lambda j: gat[h, j].reshape(256, 128)

    def whole(j):
        return jnp.concatenate([gat[0, j].reshape(256, 128), gat[1, j].reshape(256, 128)], axis=1)

    for j in (1, 3, 2):
        loans[j, 1].wait_recv()
    sends = []
    for i, h in enumerate((core, 1 - core)):
        if i == 1:
            swap.wait_recv()
        l_send[h] = message(1, half(h)).astype(BF16)
        sends.append(remote(l_send.at[h], l_recv.at[h], l_ssem.at[i], l_rsem.at[i], (a, other)))
        sends[-1].start()
    for j in (1, 3, 2):
        loans[j, 0].wait_recv()
    l_own[...] = message(0, whole)

    for c in answers:
        c.wait_recv()
    near = short[...] + sh_recv[0].astype(F32) + sh_recv[1].astype(F32)
    own = feats[pl.ds(pl.multiple_of(f * 256, 256), 256), :].astype(F32)
    l_own[...] = l_own[...] + near * (1.0 / math.sqrt(TILE)) + own
    for c in sends:
        c.wait_recv()
    far = jnp.concatenate([l_recv[0].astype(F32), l_recv[1].astype(F32)], axis=1)
    out_ref[...] = (l_own[...] + far).astype(BF16)

    pltpu.make_async_copy(parts, parts, rs_ssem).wait()
    pltpu.make_async_copy(seven, seven, az_ssem).wait()
    pltpu.make_async_copy(seven_rows, seven_rows, ap_ssem).wait()
    for c in asks + answers + sends + [swap] + list(loans.values()):
        c.wait_send()


def shards(feats, positions, phases, filt, w_value, neighbour_tiles, neighbour_count):
    n_atom = lax.axis_size("atom")
    n_freq = lax.axis_size("freq")
    scale = 1.0 / math.sqrt(feats.shape[0] * n_atom * phases.shape[2] * n_freq)
    in_hbm = pl.BlockSpec(memory_space=pltpu.HBM)
    vmem, dma = pltpu.VMEM, pltpu.SemaphoreType.DMA
    operands = [
        pltpu.with_memory_space_constraint(x, pltpu.HBM)
        for x in (feats, positions, phases, filt, w_value, neighbour_tiles, neighbour_count)
    ]
    return pl.pallas_call(
        functools.partial(kernel, scale),
        out_shape=jax.ShapeDtypeStruct((256, 256), BF16),
        in_specs=[in_hbm] * 7,
        out_specs=pl.BlockSpec(memory_space=pltpu.VMEM),
        scratch_shapes=[
            pltpu.SMEM((2, 8), jnp.int32),
            pltpu.SMEM((2,), jnp.int32),
            vmem((2048, 256), BF16),
            vmem((3, 2048), F32),
            vmem((2048, 256), BF16),
            vmem((3, 2, 256, 256), BF16),
            vmem((128, 256), F32),
            vmem((256, 256), BF16),
            vmem((2048, 256), BF16),
            vmem((256, 2048), BF16),
            vmem((8, 256), F32),
            vmem((16, 128), jnp.int32),
            vmem((2, 8, 256), F32),
            vmem((2, 16, 128), jnp.int32),
            vmem((3, 256, 128), F32),
            vmem((256, 256), F32),
            vmem((2, 256, 256), BF16),
            vmem((2, 256, 256), BF16),
            vmem((32, 16, 128), BF16),
            vmem((32, 16, 128), BF16),
            vmem((2, 4, 2, 8, 16, 128), BF16),
            vmem((256, 256), F32),
            vmem((2, 256, 128), BF16),
            vmem((2, 256, 128), BF16),
            dma((5 + 3 * CHUNKS,)),
            dma,
            dma,
            dma((6,)),
            dma((6,)),
            dma((4,)),
            dma((4,)),
            dma((2,)),
            dma((2,)),
            dma,
            dma,
            dma,
            dma,
            dma,
            dma,
            dma((2,)),
            dma((2,)),
        ],
        compiler_params=pltpu.CompilerParams(
            collective_id=0, has_side_effects=True, vmem_limit_bytes=40_000_000
        ),
    )(*operands)


def solution(mesh):
    in_specs = (
        P("atom", None),
        P(None, "atom"),
        P(None, "atom", "freq"),
        P("freq", None),
        P(),
        P(("atom", "freq"), None),
        P(("atom", "freq")),
    )
    out_specs = P(("atom", "freq"), None)
    return jax.shard_map(shards, mesh=mesh, in_specs=in_specs, out_specs=out_specs, check_vma=False)
```

```python
import functools
import math

import jax
import jax.numpy as jnp
from jax import lax
from jax.experimental import pallas as pl
from jax.experimental.pallas import tpu as pltpu
from jax.sharding import PartitionSpec as P

MESH = pl.DeviceIdType.MESH
TILE = 128
CHUNKS = 2
FAR = 1e30
LATE = ((2, 0),)
ATOM_PEERS = [(i, j, k) for j in (4, 3, 5, 2, 6, 1, 7, 0) for i in (1, 0) for k in (1, 0) if i + j + k > 0]

F32 = jnp.float32
BF16 = jnp.bfloat16


def dot(a, b):
    return jnp.dot(a, b, preferred_element_type=F32)


def kernel(
    scale,
    feats_hbm,
    pos_hbm,
    phases_hbm,
    filt_hbm,
    w_hbm,
    tiles_hbm,
    count_hbm,
    out_ref,
    tiles_smem,
    count_smem,
    feats,
    pos,
    ph,
    lent,
    filt,
    w,
    values,
    weight,
    req_pos,
    req_ids,
    in_pos,
    in_ids,
    columns,
    short,
    sh_send,
    sh_recv,
    rs_send,
    rs_recv,
    gat,
    l_own,
    l_send,
    l_recv,
    in_sem,
    rs_ssem,
    rs_rsem,
    ph_ssem,
    ph_rsem,
    rq_ssem,
    rq_rsem,
    sh_ssem,
    sh_rsem,
    az_ssem,
    az_rsem,
    ap_ssem,
    ap_rsem,
    sw_ssem,
    sw_rsem,
    l_ssem,
    l_rsem,
):
    a = lax.axis_index("atom")
    f = lax.axis_index("freq")
    core = lax.rem(a, 2)
    row = a // 2
    x_lo = row // 8
    z = lax.rem(row, 8)
    x_hi = f // 4
    y = lax.rem(f, 4)
    other = (1 - x_hi) * 4 + y

    def remote(src, dst, ssem, rsem, to):
        return pltpu.make_async_remote_copy(
            src_ref=src, dst_ref=dst, send_sem=ssem, recv_sem=rsem, device_id=to, device_id_type=MESH
        )

    z_at = [lax.rem(z + j, 8) * 2 for j in range(8)]
    x_at = [x_lo * 16, (1 - x_lo) * 16]
    core_at = [core, 1 - core]

    def block_at(d):
        return x_at[d[0]] + z_at[d[1]] + core_at[d[2]]

    barrier = pltpu.get_barrier_semaphore()

    def greet(to):
        pl.semaphore_signal(barrier, inc=1, device_id=to, device_id_type=MESH)

    for d in ATOM_PEERS:
        greet((block_at(d), f))
    for j in (2, 1, 3):
        greet((a, x_hi * 4 + lax.rem(y + j, 4)))
    greet((a, other))

    step = 2048 // CHUNKS
    loads = [
        pltpu.make_async_copy(pos_hbm, pos, in_sem.at[0]),
        pltpu.make_async_copy(filt_hbm, filt, in_sem.at[1]),
        pltpu.make_async_copy(w_hbm, w, in_sem.at[2]),
        pltpu.make_async_copy(tiles_hbm, tiles_smem, in_sem.at[3]),
        pltpu.make_async_copy(count_hbm, count_smem, in_sem.at[4]),
    ]
    chunk_loads = []
    for i in range(CHUNKS):
        rows = pl.ds(i * step, step)
        trio = [
            pltpu.make_async_copy(phases_hbm.at[0, rows], ph.at[rows, pl.ds(0, 128)], in_sem.at[5 + 3 * i]),
            pltpu.make_async_copy(phases_hbm.at[1, rows], ph.at[rows, pl.ds(128, 128)], in_sem.at[6 + 3 * i]),
            pltpu.make_async_copy(feats_hbm.at[rows], feats.at[rows], in_sem.at[7 + 3 * i]),
        ]
        for c in trio:
            c.start()
        chunk_loads.append(trio)
    for c in loads:
        c.start()

    total = None
    for i in range(CHUNKS):
        for c in chunk_loads[i]:
            c.wait()
        rows = pl.ds(i * step, step)
        part = lax.dot_general(
            ph[rows, :], feats[rows, :], (((0,), (0,)), ((), ())), preferred_element_type=F32
        )
        total = part if total is None else total + part
    for h in range(2):
        rs_send[h * 16 : (h + 1) * 16] = total[:, h * 128 : (h + 1) * 128].astype(BF16).reshape(16, 16, 128)

    loads[0].wait()
    loads[3].wait()
    loads[4].wait()
    req_pos[...] = jnp.zeros_like(req_pos)
    req_pos[0:3, :] = pos[:, pl.ds(pl.multiple_of(f * 256, 256), 256)]
    for t in range(2):
        for n in range(8):
            tile = jnp.where(n < count_smem[t], tiles_smem[t, n], -1)
            req_ids[t * 8 + n : t * 8 + n + 1, :] = jnp.full((1, 128), tile, jnp.int32)

    pl.semaphore_wait(barrier, 35)

    for i, d in enumerate(ATOM_PEERS):
        to = block_at(d)
        share_of = core_at[d[2]] * 16 + (x_at[d[0]] + z_at[d[1]]) // 2
        remote(rs_send.at[share_of], rs_recv.at[i + 1], rs_ssem, rs_rsem, (to, f)).start()
    before, after = lax.rem(a + 31, 32), lax.rem(a + 1, 32)
    asks = []
    for i, to in enumerate((before, after)):
        asks.append(remote(req_pos, in_pos.at[i], rq_ssem.at[2 * i], rq_rsem.at[2 * i], (to, f)))
        asks.append(remote(req_ids, in_ids.at[i], rq_ssem.at[2 * i + 1], rq_rsem.at[2 * i + 1], (to, f)))
    for c in asks:
        c.start()

    def lend(j, hi):
        to = lax.rem(y + j, 4)
        rows = pl.ds(pl.multiple_of((lax.rem(x_hi + hi, 2) * 4 + to) * 256, 256), 256)
        i = (j - 1) * 2 + hi
        return remote(
            ph.at[rows], lent.at[j - 1, hi], ph_ssem.at[i], ph_rsem.at[i], (a, x_hi * 4 + to)
        )

    loans = {(j, hi): lend(j, hi) for hi in (1, 0) for j in (1, 3, 2)}
    for key in loans:
        if key not in LATE:
            loans[key].start()

    loads[2].wait()
    for i in range(CHUNKS):
        rows = pl.ds(i * step, step)
        values[rows, :] = dot(feats[rows, :], w[...]).astype(BF16)

    def query(pos_ref, ids_ref):
        flipped = pos_ref[...].T
        for c in range(3):
            columns[c] = jnp.broadcast_to(flipped[:, c : c + 1], (256, 128))

        def tile(s, carry):
            lanes = pl.ds(pl.multiple_of(s * TILE, TILE), TILE)
            mine = a * 16 + s
            theirs = pos[:, lanes]
            for t in range(2):
                rows = pl.ds(t * TILE, TILE)
                live = jnp.max((ids_ref[t * 8 : (t + 1) * 8, :] == mine).astype(F32), axis=0, keepdims=True)
                dist = (1.0 - live) * FAR
                for c in range(3):
                    diff = columns[c, rows, :] - theirs[c : c + 1, :]
                    dist = dist + diff * diff
                weight[rows, lanes] = jnp.exp(-dist).astype(BF16)
            return carry

        lax.fori_loop(0, 16, tile, 0)
        return dot(weight[...], values[...])

    short[...] = query(req_pos, req_ids)

    parts = rs_recv.at[pl.ds(1, 31)]
    pltpu.make_async_copy(parts, parts, rs_rsem).wait()
    share = rs_send[core * 16 + row].astype(F32)
    share = share + jnp.sum(rs_recv[1:32].astype(F32), axis=0)
    loads[1].wait()
    k_rows = pl.ds(pl.multiple_of(lax.rem(row, 8) * 16, 16), 16)
    filt_share = jnp.where(core == 0, filt[k_rows, 0:128], filt[k_rows, 128:256])
    gat[core, 0, x_lo, z] = (filt_share * share * scale).astype(BF16)

    mine = gat.at[core, 0, x_lo, z]
    for d in ATOM_PEERS:
        if d[2] == 0:
            remote(mine, mine, az_ssem, az_rsem, (block_at(d), f)).start()

    answers = []

    def answer(i, to):
        asks[2 * i].wait_recv()
        asks[2 * i + 1].wait_recv()
        sh_send[i] = query(in_pos.at[i], in_ids.at[i]).astype(BF16)
        answers.append(remote(sh_send.at[i], sh_recv.at[i], sh_ssem.at[i], sh_rsem.at[i], (to, f)))

    answer(0, after)
    fifteen = rs_recv.at[pl.ds(1, 15)]
    pltpu.make_async_copy(fifteen, fifteen, az_rsem).wait()
    plane = []
    for j in (2, 1, 3):
        to = (a, x_hi * 4 + lax.rem(y + j, 4))
        plane.append(remote(gat.at[core, 0], gat.at[core, 4 - j], ap_ssem.at[j - 1], ap_rsem.at[j - 1], to))
        plane[-1].start()
    answers[0].start()
    answer(1, before)
    answers[1].start()
    for key in LATE:
        loans[key].start()

    def term(hi, s, filtered):
        if s == 0:
            rows = pl.ds(pl.multiple_of((lax.rem(x_hi + hi, 2) * 4 + y) * 256, 256), 256)
            return dot(ph[rows, :], filtered)
        return dot(lent[3 - s, hi], filtered)

    for j in (1, 3, 2):
        loans[j, 1].wait_recv()
    swaps = []
    first = None
    for s in (0, 1, 3, 2):
        if s:
            plane[(2, 1, 3).index(4 - s)].wait_recv()
        swaps.append(remote(gat.at[core, s], gat.at[core, s], sw_ssem.at[s], sw_rsem.at[s], (row * 2 + 1 - core, f)))
        swaps[-1].start()
        part = term(1, s, gat[core, s].reshape(256, 128))
        first = part if first is None else first + part
    l_send[core] = first.astype(BF16)
    sends = [remote(l_send.at[core], l_recv.at[core], l_ssem.at[0], l_rsem.at[0], (a, other))]
    sends[0].start()
    second = None
    for s, swap in zip((0, 1, 3, 2), swaps):
        swap.wait_recv()
        part = term(1, s, gat[1 - core, s].reshape(256, 128))
        second = part if second is None else second + part
    l_send[1 - core] = second.astype(BF16)
    sends.append(remote(l_send.at[1 - core], l_recv.at[1 - core], l_ssem.at[1], l_rsem.at[1], (a, other)))
    sends[1].start()

    mine = None
    for s in (0, 1, 3, 2):
        if s:
            loans[4 - s, 0].wait_recv()
        both = jnp.concatenate([gat[0, s].reshape(256, 128), gat[1, s].reshape(256, 128)], axis=1)
        part = term(0, s, both)
        mine = part if mine is None else mine + part
    l_own[...] = mine

    for c in answers:
        c.wait_recv()
    near = short[...] + sh_recv[0].astype(F32) + sh_recv[1].astype(F32)
    own = feats[pl.ds(pl.multiple_of(f * 256, 256), 256), :].astype(F32)
    l_own[...] = l_own[...] + near * (1.0 / math.sqrt(TILE)) + own
    for c in sends:
        c.wait_recv()
    far = jnp.concatenate([l_recv[0].astype(F32), l_recv[1].astype(F32)], axis=1)
    out_ref[...] = (l_own[...] + far).astype(BF16)

    pltpu.make_async_copy(parts, parts, rs_ssem).wait()
    pltpu.make_async_copy(fifteen, fifteen, az_ssem).wait()
    for c in asks + plane + answers + sends + swaps + list(loans.values()):
        c.wait_send()


def shards(feats, positions, phases, filt, w_value, neighbour_tiles, neighbour_count):
    n_atom = lax.axis_size("atom")
    n_freq = lax.axis_size("freq")
    scale = 1.0 / math.sqrt(feats.shape[0] * n_atom * phases.shape[2] * n_freq)
    in_hbm = pl.BlockSpec(memory_space=pltpu.HBM)
    vmem, dma = pltpu.VMEM, pltpu.SemaphoreType.DMA
    operands = [
        pltpu.with_memory_space_constraint(x, pltpu.HBM)
        for x in (feats, positions, phases, filt, w_value, neighbour_tiles, neighbour_count)
    ]
    return pl.pallas_call(
        functools.partial(kernel, scale),
        out_shape=jax.ShapeDtypeStruct((256, 256), BF16),
        in_specs=[in_hbm] * 7,
        out_specs=pl.BlockSpec(memory_space=pltpu.VMEM),
        scratch_shapes=[
            pltpu.SMEM((2, 8), jnp.int32),
            pltpu.SMEM((2,), jnp.int32),
            vmem((2048, 256), BF16),
            vmem((3, 2048), F32),
            vmem((2048, 256), BF16),
            vmem((3, 2, 256, 256), BF16),
            vmem((128, 256), F32),
            vmem((256, 256), BF16),
            vmem((2048, 256), BF16),
            vmem((256, 2048), BF16),
            vmem((8, 256), F32),
            vmem((16, 128), jnp.int32),
            vmem((2, 8, 256), F32),
            vmem((2, 16, 128), jnp.int32),
            vmem((3, 256, 128), F32),
            vmem((256, 256), F32),
            vmem((2, 256, 256), BF16),
            vmem((2, 256, 256), BF16),
            vmem((32, 16, 128), BF16),
            vmem((32, 16, 128), BF16),
            vmem((2, 4, 2, 8, 16, 128), BF16),
            vmem((256, 256), F32),
            vmem((2, 256, 128), BF16),
            vmem((2, 256, 128), BF16),
            dma((5 + 3 * CHUNKS,)),
            dma,
            dma,
            dma((6,)),
            dma((6,)),
            dma((4,)),
            dma((4,)),
            dma((2,)),
            dma((2,)),
            dma,
            dma,
            dma((3,)),
            dma((3,)),
            dma((4,)),
            dma((4,)),
            dma((2,)),
            dma((2,)),
        ],
        compiler_params=pltpu.CompilerParams(
            collective_id=0, has_side_effects=True, vmem_limit_bytes=40_000_000
        ),
    )(*operands)


def solution(mesh):
    in_specs = (
        P("atom", None),
        P(None, "atom"),
        P(None, "atom", "freq"),
        P("freq", None),
        P(),
        P(("atom", "freq"), None),
        P(("atom", "freq")),
    )
    out_specs = P(("atom", "freq"), None)
    return jax.shard_map(shards, mesh=mesh, in_specs=in_specs, out_specs=out_specs, check_vma=False)
```

```python
import functools
import math

import jax
import jax.numpy as jnp
from jax import lax
from jax.experimental import pallas as pl
from jax.experimental.pallas import tpu as pltpu
from jax.sharding import PartitionSpec as P

MESH = pl.DeviceIdType.MESH
TILE = 128
CHUNKS = 2
FAR = 1e30
LATE = ((2, 1), (1, 0), (3, 0), (2, 0))
ATOM_PEERS = [(i, j, k) for j in (4, 3, 5, 2, 6, 1, 7, 0) for i in (1, 0) for k in (1, 0) if i + j + k > 0]

F32 = jnp.float32
BF16 = jnp.bfloat16


def dot(a, b):
    return jnp.dot(a, b, preferred_element_type=F32)


def kernel(
    scale,
    feats_hbm,
    pos_hbm,
    phases_hbm,
    filt_hbm,
    w_hbm,
    tiles_hbm,
    count_hbm,
    out_ref,
    tiles_smem,
    count_smem,
    feats,
    pos,
    ph,
    lent,
    filt,
    w,
    values,
    weight,
    req_pos,
    req_ids,
    in_pos,
    in_ids,
    columns,
    short,
    sh_send,
    sh_recv,
    rs_send,
    rs_recv,
    gat,
    l_own,
    l_send,
    l_recv,
    in_sem,
    rs_ssem,
    rs_rsem,
    ph_ssem,
    ph_rsem,
    rq_ssem,
    rq_rsem,
    sh_ssem,
    sh_rsem,
    ap_ssem,
    ap_rsem,
    sw_ssem,
    sw_rsem,
    l_ssem,
    l_rsem,
):
    a = lax.axis_index("atom")
    f = lax.axis_index("freq")
    core = lax.rem(a, 2)
    row = a // 2
    x_lo = row // 8
    z = lax.rem(row, 8)
    x_hi = f // 4
    y = lax.rem(f, 4)
    other = (1 - x_hi) * 4 + y

    def remote(src, dst, ssem, rsem, to):
        return pltpu.make_async_remote_copy(
            src_ref=src, dst_ref=dst, send_sem=ssem, recv_sem=rsem, device_id=to, device_id_type=MESH
        )

    z_at = [lax.rem(z + j, 8) * 2 for j in range(8)]
    x_at = [x_lo * 16, (1 - x_lo) * 16]
    core_at = [core, 1 - core]

    def block_at(d):
        return x_at[d[0]] + z_at[d[1]] + core_at[d[2]]

    barrier = pltpu.get_barrier_semaphore()

    def greet(to):
        pl.semaphore_signal(barrier, inc=1, device_id=to, device_id_type=MESH)

    for d in ATOM_PEERS:
        greet((block_at(d), f))
    for j in (2, 1, 3):
        greet((a, x_hi * 4 + lax.rem(y + j, 4)))
    greet((a, other))

    step = 2048 // CHUNKS
    loads = [
        pltpu.make_async_copy(pos_hbm, pos, in_sem.at[0]),
        pltpu.make_async_copy(filt_hbm, filt, in_sem.at[1]),
        pltpu.make_async_copy(w_hbm, w, in_sem.at[2]),
        pltpu.make_async_copy(tiles_hbm, tiles_smem, in_sem.at[3]),
        pltpu.make_async_copy(count_hbm, count_smem, in_sem.at[4]),
    ]
    chunk_loads = []
    for i in range(CHUNKS):
        rows = pl.ds(i * step, step)
        trio = [
            pltpu.make_async_copy(phases_hbm.at[0, rows], ph.at[rows, pl.ds(0, 128)], in_sem.at[5 + 3 * i]),
            pltpu.make_async_copy(phases_hbm.at[1, rows], ph.at[rows, pl.ds(128, 128)], in_sem.at[6 + 3 * i]),
            pltpu.make_async_copy(feats_hbm.at[rows], feats.at[rows], in_sem.at[7 + 3 * i]),
        ]
        for c in trio:
            c.start()
        chunk_loads.append(trio)
    for c in loads:
        c.start()

    total = None
    for i in range(CHUNKS):
        for c in chunk_loads[i]:
            c.wait()
        rows = pl.ds(i * step, step)
        part = lax.dot_general(
            ph[rows, :], feats[rows, :], (((0,), (0,)), ((), ())), preferred_element_type=F32
        )
        total = part if total is None else total + part
    for h in range(2):
        rs_send[h * 16 : (h + 1) * 16] = total[:, h * 128 : (h + 1) * 128].astype(BF16).reshape(16, 16, 128)

    loads[0].wait()
    loads[3].wait()
    loads[4].wait()
    req_pos[...] = jnp.zeros_like(req_pos)
    req_pos[0:3, :] = pos[:, pl.ds(pl.multiple_of(f * 256, 256), 256)]
    for t in range(2):
        for n in range(8):
            tile = jnp.where(n < count_smem[t], tiles_smem[t, n], -1)
            req_ids[t * 8 + n : t * 8 + n + 1, :] = jnp.full((1, 128), tile, jnp.int32)

    pl.semaphore_wait(barrier, 35)

    for i, d in enumerate(ATOM_PEERS):
        to = block_at(d)
        share_of = core_at[d[2]] * 16 + (x_at[d[0]] + z_at[d[1]]) // 2
        remote(rs_send.at[share_of], rs_recv.at[i + 1], rs_ssem, rs_rsem, (to, f)).start()
    before, after = lax.rem(a + 31, 32), lax.rem(a + 1, 32)
    asks = []
    for i, to in enumerate((before, after)):
        asks.append(remote(req_pos, in_pos.at[i], rq_ssem.at[2 * i], rq_rsem.at[2 * i], (to, f)))
        asks.append(remote(req_ids, in_ids.at[i], rq_ssem.at[2 * i + 1], rq_rsem.at[2 * i + 1], (to, f)))
    for c in asks:
        c.start()

    def lend(j, hi):
        to = lax.rem(y + j, 4)
        rows = pl.ds(pl.multiple_of((lax.rem(x_hi + hi, 2) * 4 + to) * 256, 256), 256)
        i = (j - 1) * 2 + hi
        return remote(
            ph.at[rows], lent.at[j - 1, hi], ph_ssem.at[i], ph_rsem.at[i], (a, x_hi * 4 + to)
        )

    loans = {(j, hi): lend(j, hi) for hi in (1, 0) for j in (1, 3, 2)}
    for key in loans:
        if key not in LATE:
            loans[key].start()

    loads[2].wait()
    for i in range(CHUNKS):
        rows = pl.ds(i * step, step)
        values[rows, :] = dot(feats[rows, :], w[...]).astype(BF16)

    def query(pos_ref, ids_ref):
        flipped = pos_ref[...].T
        for c in range(3):
            columns[c] = jnp.broadcast_to(flipped[:, c : c + 1], (256, 128))

        def tile(s, carry):
            lanes = pl.ds(pl.multiple_of(s * TILE, TILE), TILE)
            mine = a * 16 + s
            theirs = pos[:, lanes]
            for t in range(2):
                rows = pl.ds(t * TILE, TILE)
                live = jnp.max((ids_ref[t * 8 : (t + 1) * 8, :] == mine).astype(F32), axis=0, keepdims=True)
                dist = (1.0 - live) * FAR
                for c in range(3):
                    diff = columns[c, rows, :] - theirs[c : c + 1, :]
                    dist = dist + diff * diff
                weight[rows, lanes] = jnp.exp(-dist).astype(BF16)
            return carry

        lax.fori_loop(0, 16, tile, 0)
        return dot(weight[...], values[...])

    short[...] = query(req_pos, req_ids)

    parts = rs_recv.at[pl.ds(1, 31)]
    pltpu.make_async_copy(parts, parts, rs_rsem).wait()
    share = rs_send[core * 16 + row].astype(F32)
    share = share + jnp.sum(rs_recv[1:32].astype(F32), axis=0)
    loads[1].wait()
    k_rows = pl.ds(pl.multiple_of(lax.rem(row, 8) * 16, 16), 16)
    filt_share = jnp.where(core == 0, filt[k_rows, 0:128], filt[k_rows, 128:256])
    gat[core, 0, x_lo, z] = (filt_share * share * scale).astype(BF16)

    y_at = [x_hi * 4 + lax.rem(y + j, 4) for j in range(4)]
    for dz in (4, 3, 5, 2, 6, 1, 7, 0):
        for j in (2, 1, 3, 0):
            for i in (1, 0):
                if dz + j + i > 0:
                    slot = (4 - j) % 4
                    remote(
                        gat.at[core, 0, x_lo, z],
                        gat.at[core, slot, x_lo, z],
                        ap_ssem.at[slot],
                        ap_rsem.at[slot],
                        (x_at[i] + z_at[dz] + core, y_at[j]),
                    ).start()

    for key in LATE:
        loans[key].start()

    answers = []

    def answer(i, to):
        asks[2 * i].wait_recv()
        asks[2 * i + 1].wait_recv()
        sh_send[i] = query(in_pos.at[i], in_ids.at[i]).astype(BF16)
        answers.append(remote(sh_send.at[i], sh_recv.at[i], sh_ssem.at[i], sh_rsem.at[i], (to, f)))

    answer(0, after)
    answer(1, before)

    def term(hi, s, filtered):
        if s == 0:
            rows = pl.ds(pl.multiple_of((lax.rem(x_hi + hi, 2) * 4 + y) * 256, 256), 256)
            return dot(ph[rows, :], filtered)
        return dot(lent[3 - s, hi], filtered)

    for j in (1, 3, 2):
        loans[j, 1].wait_recv()
    swaps = []
    first = None
    for s in (0, 1, 3, 2):
        arrived = rs_recv.at[pl.ds(1, 16 if s else 15)]
        pltpu.make_async_copy(arrived, arrived, ap_rsem.at[s]).wait()
        swaps.append(remote(gat.at[core, s], gat.at[core, s], sw_ssem.at[s], sw_rsem.at[s], (row * 2 + 1 - core, f)))
        swaps[-1].start()
        part = term(1, s, gat[core, s].reshape(256, 128))
        first = part if first is None else first + part
    l_send[core] = first.astype(BF16)
    sends = [remote(l_send.at[core], l_recv.at[core], l_ssem.at[0], l_rsem.at[0], (a, other))]
    sends[0].start()
    for c in answers:
        c.start()
    second = None
    for s, swap in zip((0, 1, 3, 2), swaps):
        swap.wait_recv()
        part = term(1, s, gat[1 - core, s].reshape(256, 128))
        second = part if second is None else second + part
    l_send[1 - core] = second.astype(BF16)
    sends.append(remote(l_send.at[1 - core], l_recv.at[1 - core], l_ssem.at[1], l_rsem.at[1], (a, other)))
    sends[1].start()

    mine = None
    for s in (0, 1, 3, 2):
        if s:
            loans[4 - s, 0].wait_recv()
        both = jnp.concatenate([gat[0, s].reshape(256, 128), gat[1, s].reshape(256, 128)], axis=1)
        part = term(0, s, both)
        mine = part if mine is None else mine + part
    l_own[...] = mine

    for c in answers:
        c.wait_recv()
    near = short[...] + sh_recv[0].astype(F32) + sh_recv[1].astype(F32)
    own = feats[pl.ds(pl.multiple_of(f * 256, 256), 256), :].astype(F32)
    l_own[...] = l_own[...] + near * (1.0 / math.sqrt(TILE)) + own
    for c in sends:
        c.wait_recv()
    far = jnp.concatenate([l_recv[0].astype(F32), l_recv[1].astype(F32)], axis=1)
    out_ref[...] = (l_own[...] + far).astype(BF16)

    pltpu.make_async_copy(parts, parts, rs_ssem).wait()
    for s in range(4):
        left = rs_recv.at[pl.ds(1, 16 if s else 15)]
        pltpu.make_async_copy(left, left, ap_ssem.at[s]).wait()
    for c in asks + answers + sends + swaps + list(loans.values()):
        c.wait_send()


def shards(feats, positions, phases, filt, w_value, neighbour_tiles, neighbour_count):
    n_atom = lax.axis_size("atom")
    n_freq = lax.axis_size("freq")
    scale = 1.0 / math.sqrt(feats.shape[0] * n_atom * phases.shape[2] * n_freq)
    in_hbm = pl.BlockSpec(memory_space=pltpu.HBM)
    vmem, dma = pltpu.VMEM, pltpu.SemaphoreType.DMA
    operands = [
        pltpu.with_memory_space_constraint(x, pltpu.HBM)
        for x in (feats, positions, phases, filt, w_value, neighbour_tiles, neighbour_count)
    ]
    return pl.pallas_call(
        functools.partial(kernel, scale),
        out_shape=jax.ShapeDtypeStruct((256, 256), BF16),
        in_specs=[in_hbm] * 7,
        out_specs=pl.BlockSpec(memory_space=pltpu.VMEM),
        scratch_shapes=[
            pltpu.SMEM((2, 8), jnp.int32),
            pltpu.SMEM((2,), jnp.int32),
            vmem((2048, 256), BF16),
            vmem((3, 2048), F32),
            vmem((2048, 256), BF16),
            vmem((3, 2, 256, 256), BF16),
            vmem((128, 256), F32),
            vmem((256, 256), BF16),
            vmem((2048, 256), BF16),
            vmem((256, 2048), BF16),
            vmem((8, 256), F32),
            vmem((16, 128), jnp.int32),
            vmem((2, 8, 256), F32),
            vmem((2, 16, 128), jnp.int32),
            vmem((3, 256, 128), F32),
            vmem((256, 256), F32),
            vmem((2, 256, 256), BF16),
            vmem((2, 256, 256), BF16),
            vmem((32, 16, 128), BF16),
            vmem((32, 16, 128), BF16),
            vmem((2, 4, 2, 8, 16, 128), BF16),
            vmem((256, 256), F32),
            vmem((2, 256, 128), BF16),
            vmem((2, 256, 128), BF16),
            dma((5 + 3 * CHUNKS,)),
            dma,
            dma,
            dma((6,)),
            dma((6,)),
            dma((4,)),
            dma((4,)),
            dma((2,)),
            dma((2,)),
            dma((4,)),
            dma((4,)),
            dma((4,)),
            dma((4,)),
            dma((2,)),
            dma((2,)),
        ],
        compiler_params=pltpu.CompilerParams(
            collective_id=0, has_side_effects=True, vmem_limit_bytes=40_000_000
        ),
    )(*operands)


def solution(mesh):
    in_specs = (
        P("atom", None),
        P(None, "atom"),
        P(None, "atom", "freq"),
        P("freq", None),
        P(),
        P(("atom", "freq"), None),
        P(("atom", "freq")),
    )
    out_specs = P(("atom", "freq"), None)
    return jax.shard_map(shards, mesh=mesh, in_specs=in_specs, out_specs=out_specs, check_vma=False)
```

```python
import functools
import math

import jax
import jax.numpy as jnp
from jax import lax
from jax.experimental import pallas as pl
from jax.experimental.pallas import tpu as pltpu
from jax.sharding import PartitionSpec as P

MESH = pl.DeviceIdType.MESH
TILE = 128
CHUNKS = 2
FAR = 1e30
LATE = ((2, 0),)
ATOM_PEERS = [(i, j, k) for j in (4, 3, 5, 2, 6, 1, 7, 0) for i in (1, 0) for k in (1, 0) if i + j + k > 0]

F32 = jnp.float32
BF16 = jnp.bfloat16


def dot(a, b):
    return jnp.dot(a, b, preferred_element_type=F32)


def kernel(
    scale,
    feats_hbm,
    pos_hbm,
    phases_hbm,
    filt_hbm,
    w_hbm,
    tiles_hbm,
    count_hbm,
    out_ref,
    tiles_smem,
    count_smem,
    feats,
    pos,
    ph,
    lent,
    seen,
    filt,
    w,
    values,
    weight,
    req_pos,
    req_ids,
    in_pos,
    in_ids,
    columns,
    short,
    sh_send,
    sh_recv,
    rs_send,
    rs_recv,
    gat,
    l_own,
    l_send,
    l_recv,
    in_sem,
    rs_ssem,
    rs_rsem,
    ph_ssem,
    ph_rsem,
    se_ssem,
    se_rsem,
    rq_ssem,
    rq_rsem,
    sh_ssem,
    sh_rsem,
    ap_ssem,
    ap_rsem,
    sw_ssem,
    sw_rsem,
    l_ssem,
    l_rsem,
):
    a = lax.axis_index("atom")
    f = lax.axis_index("freq")
    core = lax.rem(a, 2)
    row = a // 2
    x_lo = row // 8
    z = lax.rem(row, 8)
    x_hi = f // 4
    y = lax.rem(f, 4)
    other = (1 - x_hi) * 4 + y

    def remote(src, dst, ssem, rsem, to):
        return pltpu.make_async_remote_copy(
            src_ref=src, dst_ref=dst, send_sem=ssem, recv_sem=rsem, device_id=to, device_id_type=MESH
        )

    z_at = [lax.rem(z + j, 8) * 2 for j in range(8)]
    x_at = [x_lo * 16, (1 - x_lo) * 16]
    core_at = [core, 1 - core]

    def block_at(d):
        return x_at[d[0]] + z_at[d[1]] + core_at[d[2]]

    barrier = pltpu.get_barrier_semaphore()

    def greet(to):
        pl.semaphore_signal(barrier, inc=1, device_id=to, device_id_type=MESH)

    for d in ATOM_PEERS:
        greet((block_at(d), f))
    for j in (2, 1, 3):
        greet((a, x_hi * 4 + lax.rem(y + j, 4)))
    greet((a, other))

    step = 2048 // CHUNKS
    loads = [
        pltpu.make_async_copy(pos_hbm, pos, in_sem.at[0]),
        pltpu.make_async_copy(filt_hbm, filt, in_sem.at[1]),
        pltpu.make_async_copy(w_hbm, w, in_sem.at[2]),
        pltpu.make_async_copy(tiles_hbm, tiles_smem, in_sem.at[3]),
        pltpu.make_async_copy(count_hbm, count_smem, in_sem.at[4]),
    ]
    chunk_loads = []
    for i in range(CHUNKS):
        rows = pl.ds(i * step, step)
        trio = [
            pltpu.make_async_copy(phases_hbm.at[0, rows], ph.at[rows, pl.ds(0, 128)], in_sem.at[5 + 3 * i]),
            pltpu.make_async_copy(phases_hbm.at[1, rows], ph.at[rows, pl.ds(128, 128)], in_sem.at[6 + 3 * i]),
            pltpu.make_async_copy(feats_hbm.at[rows], feats.at[rows], in_sem.at[7 + 3 * i]),
        ]
        for c in trio:
            c.start()
        chunk_loads.append(trio)
    for c in loads:
        c.start()

    total = None
    for i in range(CHUNKS):
        for c in chunk_loads[i]:
            c.wait()
        rows = pl.ds(i * step, step)
        part = lax.dot_general(
            ph[rows, :], feats[rows, :], (((0,), (0,)), ((), ())), preferred_element_type=F32
        )
        total = part if total is None else total + part
    for h in range(2):
        rs_send[h * 16 : (h + 1) * 16] = total[:, h * 128 : (h + 1) * 128].astype(BF16).reshape(16, 16, 128)

    loads[0].wait()
    loads[3].wait()
    loads[4].wait()
    req_pos[...] = jnp.zeros_like(req_pos)
    req_pos[0:3, :] = pos[:, pl.ds(pl.multiple_of(f * 256, 256), 256)]
    for t in range(2):
        for n in range(8):
            tile = jnp.where(n < count_smem[t], tiles_smem[t, n], -1)
            req_ids[t * 8 + n : t * 8 + n + 1, :] = jnp.full((1, 128), tile, jnp.int32)

    pl.semaphore_wait(barrier, 35)

    for i, d in enumerate(ATOM_PEERS):
        to = block_at(d)
        share_of = core_at[d[2]] * 16 + (x_at[d[0]] + z_at[d[1]]) // 2
        remote(rs_send.at[share_of], rs_recv.at[i + 1], rs_ssem, rs_rsem, (to, f)).start()
    before, after = lax.rem(a + 31, 32), lax.rem(a + 1, 32)
    asks = []
    for i, to in enumerate((before, after)):
        asks.append(remote(req_pos, in_pos.at[i], rq_ssem.at[2 * i], rq_rsem.at[2 * i], (to, f)))
        asks.append(remote(req_ids, in_ids.at[i], rq_ssem.at[2 * i + 1], rq_rsem.at[2 * i + 1], (to, f)))
    for c in asks:
        c.start()

    def lend(j, hi):
        to = lax.rem(y + j, 4)
        rows = pl.ds(pl.multiple_of((lax.rem(x_hi + hi, 2) * 4 + to) * 256, 256), 256)
        i = (j - 1) * 2 + hi
        return remote(
            ph.at[rows], lent.at[j - 1, hi], ph_ssem.at[i], ph_rsem.at[i], (a, x_hi * 4 + to)
        )

    loans = {(j, hi): lend(j, hi) for hi in (1, 0) for j in (1, 3, 2)}
    for key in loans:
        if key not in LATE:
            loans[key].start()

    loads[2].wait()
    for i in range(CHUNKS):
        rows = pl.ds(i * step, step)
        values[rows, :] = dot(feats[rows, :], w[...]).astype(BF16)

    def query(pos_ref, ids_ref):
        flipped = pos_ref[...].T
        for c in range(3):
            columns[c] = jnp.broadcast_to(flipped[:, c : c + 1], (256, 128))

        def tile(s, carry):
            lanes = pl.ds(pl.multiple_of(s * TILE, TILE), TILE)
            mine = a * 16 + s
            theirs = pos[:, lanes]
            for t in range(2):
                rows = pl.ds(t * TILE, TILE)
                live = jnp.max((ids_ref[t * 8 : (t + 1) * 8, :] == mine).astype(F32), axis=0, keepdims=True)
                dist = (1.0 - live) * FAR
                for c in range(3):
                    diff = columns[c, rows, :] - theirs[c : c + 1, :]
                    dist = dist + diff * diff
                weight[rows, lanes] = jnp.exp(-dist).astype(BF16)
            return carry

        lax.fori_loop(0, 16, tile, 0)
        return dot(weight[...], values[...])

    short[...] = query(req_pos, req_ids)

    parts = rs_recv.at[pl.ds(1, 31)]
    pltpu.make_async_copy(parts, parts, rs_rsem).wait()
    share = rs_send[core * 16 + row].astype(F32)
    share = share + jnp.sum(rs_recv[1:32].astype(F32), axis=0)
    loads[1].wait()
    k_rows = pl.ds(pl.multiple_of(lax.rem(row, 8) * 16, 16), 16)
    filt_share = jnp.where(core == 0, filt[k_rows, 0:128], filt[k_rows, 128:256])
    gat[core, 0, x_lo, z] = (filt_share * share * scale).astype(BF16)

    y_at = [x_hi * 4 + lax.rem(y + j, 4) for j in range(4)]
    for dz in (4, 3, 5, 2, 6, 1, 7, 0):
        for j in (2, 1, 3, 0):
            for i in (1, 0):
                if dz + j + i > 0:
                    slot = (4 - j) % 4
                    remote(
                        gat.at[core, 0, x_lo, z],
                        gat.at[core, slot, x_lo, z],
                        ap_ssem.at[slot],
                        ap_rsem.at[slot],
                        (x_at[i] + z_at[dz] + core, y_at[j]),
                    ).start()

    for key in LATE:
        loans[key].start()

    answers = []

    def answer(i, to):
        asks[2 * i].wait_recv()
        asks[2 * i + 1].wait_recv()
        sh_send[i] = query(in_pos.at[i], in_ids.at[i]).astype(BF16)
        answers.append(remote(sh_send.at[i], sh_recv.at[i], sh_ssem.at[i], sh_rsem.at[i], (to, f)))

    answer(0, after)
    answers[0].start()
    answer(1, before)
    answers[1].start()

    twin_rows = pl.ds(pl.multiple_of(((1 - x_hi) * 4 + y) * 256, 256), 256)
    mate = (row * 2 + 1 - core, f)
    shown = [remote(ph.at[twin_rows], seen.at[0], se_ssem.at[0], se_rsem.at[0], mate)]
    shown[0].start()
    for j in (1, 3, 2):
        loans[j, 1].wait_recv()
        s = 4 - j
        shown.append(remote(lent.at[j - 1, 1], seen.at[s], se_ssem.at[s], se_rsem.at[s], mate))
        shown[-1].start()

    swaps = []
    here = there = None
    for i, s in enumerate((0, 3, 1, 2)):
        shown[i].wait_recv()
        arrived = rs_recv.at[pl.ds(1, 16 if s else 15)]
        pltpu.make_async_copy(arrived, arrived, ap_rsem.at[s]).wait()
        swaps.append(remote(gat.at[core, s], gat.at[core, s], sw_ssem.at[s], sw_rsem.at[s], mate))
        swaps[i].start()
        filtered = gat[core, s].reshape(256, 128)
        part = dot(lent[3 - s, 1] if s else ph[twin_rows, :], filtered)
        here = part if here is None else here + part
        part = dot(seen[s], filtered)
        there = part if there is None else there + part
    l_send[0] = here.astype(BF16)
    sends = [remote(l_send.at[0], l_recv.at[core], l_ssem.at[0], l_rsem.at[0], (a, other))]
    sends[0].start()
    l_send[1] = there.astype(BF16)
    sends.append(remote(l_send.at[1], l_recv.at[core], l_ssem.at[1], l_rsem.at[1], (mate[0], other)))
    sends[1].start()

    own_rows = pl.ds(pl.multiple_of(f * 256, 256), 256)
    mine = None
    for s in (0, 3, 1, 2):
        swaps[(0, 3, 1, 2).index(s)].wait_recv()
        if s:
            loans[4 - s, 0].wait_recv()
        both = jnp.concatenate([gat[0, s].reshape(256, 128), gat[1, s].reshape(256, 128)], axis=1)
        part = dot(lent[3 - s, 0] if s else ph[own_rows, :], both)
        mine = part if mine is None else mine + part
    l_own[...] = mine

    for c in answers:
        c.wait_recv()
    near = short[...] + sh_recv[0].astype(F32) + sh_recv[1].astype(F32)
    own = feats[own_rows, :].astype(F32)
    l_own[...] = l_own[...] + near * (1.0 / math.sqrt(TILE)) + own
    for c in sends:
        c.wait_recv()
    far = jnp.concatenate([l_recv[0].astype(F32), l_recv[1].astype(F32)], axis=1)
    out_ref[...] = (l_own[...] + far).astype(BF16)

    pltpu.make_async_copy(parts, parts, rs_ssem).wait()
    for s in range(4):
        left = rs_recv.at[pl.ds(1, 16 if s else 15)]
        pltpu.make_async_copy(left, left, ap_ssem.at[s]).wait()
    for c in asks + answers + shown + sends + swaps + list(loans.values()):
        c.wait_send()


def shards(feats, positions, phases, filt, w_value, neighbour_tiles, neighbour_count):
    n_atom = lax.axis_size("atom")
    n_freq = lax.axis_size("freq")
    scale = 1.0 / math.sqrt(feats.shape[0] * n_atom * phases.shape[2] * n_freq)
    in_hbm = pl.BlockSpec(memory_space=pltpu.HBM)
    vmem, dma = pltpu.VMEM, pltpu.SemaphoreType.DMA
    operands = [
        pltpu.with_memory_space_constraint(x, pltpu.HBM)
        for x in (feats, positions, phases, filt, w_value, neighbour_tiles, neighbour_count)
    ]
    return pl.pallas_call(
        functools.partial(kernel, scale),
        out_shape=jax.ShapeDtypeStruct((256, 256), BF16),
        in_specs=[in_hbm] * 7,
        out_specs=pl.BlockSpec(memory_space=pltpu.VMEM),
        scratch_shapes=[
            pltpu.SMEM((2, 8), jnp.int32),
            pltpu.SMEM((2,), jnp.int32),
            vmem((2048, 256), BF16),
            vmem((3, 2048), F32),
            vmem((2048, 256), BF16),
            vmem((3, 2, 256, 256), BF16),
            vmem((4, 256, 256), BF16),
            vmem((128, 256), F32),
            vmem((256, 256), BF16),
            vmem((2048, 256), BF16),
            vmem((256, 2048), BF16),
            vmem((8, 256), F32),
            vmem((16, 128), jnp.int32),
            vmem((2, 8, 256), F32),
            vmem((2, 16, 128), jnp.int32),
            vmem((3, 256, 128), F32),
            vmem((256, 256), F32),
            vmem((2, 256, 256), BF16),
            vmem((2, 256, 256), BF16),
            vmem((32, 16, 128), BF16),
            vmem((32, 16, 128), BF16),
            vmem((2, 4, 2, 8, 16, 128), BF16),
            vmem((256, 256), F32),
            vmem((2, 256, 128), BF16),
            vmem((2, 256, 128), BF16),
            dma((5 + 3 * CHUNKS,)),
            dma,
            dma,
            dma((6,)),
            dma((6,)),
            dma((4,)),
            dma((4,)),
            dma((4,)),
            dma((4,)),
            dma((2,)),
            dma((2,)),
            dma((4,)),
            dma((4,)),
            dma((4,)),
            dma((4,)),
            dma((2,)),
            dma((2,)),
        ],
        compiler_params=pltpu.CompilerParams(
            collective_id=0, has_side_effects=True, vmem_limit_bytes=40_000_000
        ),
    )(*operands)


def solution(mesh):
    in_specs = (
        P("atom", None),
        P(None, "atom"),
        P(None, "atom", "freq"),
        P("freq", None),
        P(),
        P(("atom", "freq"), None),
        P(("atom", "freq")),
    )
    out_specs = P(("atom", "freq"), None)
    return jax.shard_map(shards, mesh=mesh, in_specs=in_specs, out_specs=out_specs, check_vma=False)
```

```python
import functools
import math

import jax
import jax.numpy as jnp
from jax import lax
from jax.experimental import pallas as pl
from jax.experimental.pallas import tpu as pltpu
from jax.sharding import PartitionSpec as P

MESH = pl.DeviceIdType.MESH
TILE = 128
CHUNKS = 2
FAR = 1e30
LATE = ((2, 0),)
ATOM_PEERS = [(i, j, k) for j in (4, 3, 5, 2, 6, 1, 7, 0) for i in (1, 0) for k in (1, 0) if i + j + k > 0]

F32 = jnp.float32
BF16 = jnp.bfloat16


def dot(a, b):
    return jnp.dot(a, b, preferred_element_type=F32)


def kernel(
    scale,
    feats_hbm,
    pos_hbm,
    phases_hbm,
    filt_hbm,
    w_hbm,
    tiles_hbm,
    count_hbm,
    out_ref,
    tiles_smem,
    count_smem,
    feats,
    pos,
    ph,
    lent,
    seen,
    filt,
    w,
    values,
    weight,
    req_pos,
    req_ids,
    in_pos,
    in_ids,
    columns,
    short,
    sh_send,
    sh_recv,
    rs_send,
    rs_recv,
    gat,
    l_own,
    l_send,
    l_recv,
    in_sem,
    rs_ssem,
    rs_rsem,
    ph_ssem,
    ph_rsem,
    se_ssem,
    se_rsem,
    rq_ssem,
    rq_rsem,
    sh_ssem,
    sh_rsem,
    ap_ssem,
    ap_rsem,
    sw_ssem,
    sw_rsem,
    l_ssem,
    l_rsem,
):
    a = lax.axis_index("atom")
    f = lax.axis_index("freq")
    core = lax.rem(a, 2)
    row = a // 2
    x_lo = row // 8
    z = lax.rem(row, 8)
    x_hi = f // 4
    y = lax.rem(f, 4)
    other = (1 - x_hi) * 4 + y

    def remote(src, dst, ssem, rsem, to):
        return pltpu.make_async_remote_copy(
            src_ref=src, dst_ref=dst, send_sem=ssem, recv_sem=rsem, device_id=to, device_id_type=MESH
        )

    z_at = [lax.rem(z + j, 8) * 2 for j in range(8)]
    x_at = [x_lo * 16, (1 - x_lo) * 16]
    core_at = [core, 1 - core]

    def block_at(d):
        return x_at[d[0]] + z_at[d[1]] + core_at[d[2]]

    barrier = pltpu.get_barrier_semaphore()

    def greet(to):
        pl.semaphore_signal(barrier, inc=1, device_id=to, device_id_type=MESH)

    for d in ATOM_PEERS:
        greet((block_at(d), f))
    for j in (2, 1, 3):
        greet((a, x_hi * 4 + lax.rem(y + j, 4)))
    greet((a, other))

    step = 2048 // CHUNKS
    loads = [
        pltpu.make_async_copy(pos_hbm, pos, in_sem.at[0]),
        pltpu.make_async_copy(filt_hbm, filt, in_sem.at[1]),
        pltpu.make_async_copy(w_hbm, w, in_sem.at[2]),
        pltpu.make_async_copy(tiles_hbm, tiles_smem, in_sem.at[3]),
        pltpu.make_async_copy(count_hbm, count_smem, in_sem.at[4]),
    ]
    chunk_loads = []
    for i in range(CHUNKS):
        rows = pl.ds(i * step, step)
        trio = [
            pltpu.make_async_copy(phases_hbm.at[0, rows], ph.at[rows, pl.ds(0, 128)], in_sem.at[5 + 3 * i]),
            pltpu.make_async_copy(phases_hbm.at[1, rows], ph.at[rows, pl.ds(128, 128)], in_sem.at[6 + 3 * i]),
            pltpu.make_async_copy(feats_hbm.at[rows], feats.at[rows], in_sem.at[7 + 3 * i]),
        ]
        for c in trio:
            c.start()
        chunk_loads.append(trio)
    for c in loads:
        c.start()

    total = None
    for i in range(CHUNKS):
        for c in chunk_loads[i]:
            c.wait()
        rows = pl.ds(i * step, step)
        part = lax.dot_general(
            ph[rows, :], feats[rows, :], (((0,), (0,)), ((), ())), preferred_element_type=F32
        )
        total = part if total is None else total + part
    for h in range(2):
        rs_send[h * 16 : (h + 1) * 16] = total[:, h * 128 : (h + 1) * 128].astype(BF16).reshape(16, 16, 128)

    loads[0].wait()
    loads[3].wait()
    loads[4].wait()
    req_pos[...] = jnp.zeros_like(req_pos)
    req_pos[0:3, :] = pos[:, pl.ds(pl.multiple_of(f * 256, 256), 256)]
    for t in range(2):
        for n in range(8):
            tile = jnp.where(n < count_smem[t], tiles_smem[t, n], -1)
            req_ids[t * 8 + n : t * 8 + n + 1, :] = jnp.full((1, 128), tile, jnp.int32)

    pl.semaphore_wait(barrier, 35)

    for i, d in enumerate(ATOM_PEERS):
        to = block_at(d)
        share_of = core_at[d[2]] * 16 + (x_at[d[0]] + z_at[d[1]]) // 2
        remote(rs_send.at[share_of], rs_recv.at[i + 1], rs_ssem, rs_rsem, (to, f)).start()
    before, after = lax.rem(a + 31, 32), lax.rem(a + 1, 32)
    asks = []
    for i, to in enumerate((before, after)):
        asks.append(remote(req_pos, in_pos.at[i], rq_ssem.at[2 * i], rq_rsem.at[2 * i], (to, f)))
        asks.append(remote(req_ids, in_ids.at[i], rq_ssem.at[2 * i + 1], rq_rsem.at[2 * i + 1], (to, f)))
    for c in asks:
        c.start()

    def lend(j, hi):
        to = lax.rem(y + j, 4)
        rows = pl.ds(pl.multiple_of((lax.rem(x_hi + hi, 2) * 4 + to) * 256, 256), 256)
        i = (j - 1) * 2 + hi
        return remote(
            ph.at[rows], lent.at[j - 1, hi], ph_ssem.at[i], ph_rsem.at[i], (a, x_hi * 4 + to)
        )

    loans = {(j, hi): lend(j, hi) for hi in (1, 0) for j in (1, 3, 2)}
    for key in loans:
        if key not in LATE:
            loans[key].start()

    loads[2].wait()
    for i in range(CHUNKS):
        rows = pl.ds(i * step, step)
        values[rows, :] = dot(feats[rows, :], w[...]).astype(BF16)

    def query(pos_ref, ids_ref):
        flipped = pos_ref[...].T
        for c in range(3):
            columns[c] = jnp.broadcast_to(flipped[:, c : c + 1], (256, 128))

        def tile(s, carry):
            lanes = pl.ds(pl.multiple_of(s * TILE, TILE), TILE)
            mine = a * 16 + s
            theirs = pos[:, lanes]
            for t in range(2):
                rows = pl.ds(t * TILE, TILE)
                live = jnp.max((ids_ref[t * 8 : (t + 1) * 8, :] == mine).astype(F32), axis=0, keepdims=True)
                dist = (1.0 - live) * FAR
                for c in range(3):
                    diff = columns[c, rows, :] - theirs[c : c + 1, :]
                    dist = dist + diff * diff
                weight[rows, lanes] = jnp.exp(-dist).astype(BF16)
            return carry

        lax.fori_loop(0, 16, tile, 0)
        return dot(weight[...], values[...])

    short[...] = query(req_pos, req_ids)

    parts = rs_recv.at[pl.ds(1, 31)]
    pltpu.make_async_copy(parts, parts, rs_rsem).wait()
    share = rs_send[core * 16 + row].astype(F32)
    share = share + jnp.sum(rs_recv[1:32].astype(F32), axis=0)
    loads[1].wait()
    k_rows = pl.ds(pl.multiple_of(lax.rem(row, 8) * 16, 16), 16)
    filt_share = jnp.where(core == 0, filt[k_rows, 0:128], filt[k_rows, 128:256])
    gat[core, 0, x_lo, z] = (filt_share * share * scale).astype(BF16)

    y_at = [x_hi * 4 + lax.rem(y + j, 4) for j in range(4)]
    for j in (2, 1, 3, 0):
        for dz in (4, 3, 5, 2, 6, 1, 7, 0):
            for i in (1, 0):
                if dz + j + i > 0:
                    slot = (4 - j) % 4
                    remote(
                        gat.at[core, 0, x_lo, z],
                        gat.at[core, slot, x_lo, z],
                        ap_ssem.at[slot],
                        ap_rsem.at[slot],
                        (x_at[i] + z_at[dz] + core, y_at[j]),
                    ).start()

    for key in LATE:
        loans[key].start()

    answers = []

    def answer(i, to):
        asks[2 * i].wait_recv()
        asks[2 * i + 1].wait_recv()
        sh_send[i] = query(in_pos.at[i], in_ids.at[i]).astype(BF16)
        answers.append(remote(sh_send.at[i], sh_recv.at[i], sh_ssem.at[i], sh_rsem.at[i], (to, f)))

    answer(0, after)
    answers[0].start()
    answer(1, before)
    answers[1].start()

    twin_rows = pl.ds(pl.multiple_of(((1 - x_hi) * 4 + y) * 256, 256), 256)
    mate = (row * 2 + 1 - core, f)
    shown = [remote(ph.at[twin_rows], seen.at[0], se_ssem.at[0], se_rsem.at[0], mate)]
    shown[0].start()
    for j in (1, 3, 2):
        loans[j, 1].wait_recv()
        s = 4 - j
        shown.append(remote(lent.at[j - 1, 1], seen.at[s], se_ssem.at[s], se_rsem.at[s], mate))
        shown[-1].start()

    swaps = []
    here = there = None
    for i, s in enumerate((0, 3, 1, 2)):
        shown[i].wait_recv()
        arrived = rs_recv.at[pl.ds(1, 16 if s else 15)]
        pltpu.make_async_copy(arrived, arrived, ap_rsem.at[s]).wait()
        swaps.append(remote(gat.at[core, s], gat.at[core, s], sw_ssem.at[s], sw_rsem.at[s], mate))
        swaps[i].start()
        filtered = gat[core, s].reshape(256, 128)
        part = dot(lent[3 - s, 1] if s else ph[twin_rows, :], filtered)
        here = part if here is None else here + part
        part = dot(seen[s], filtered)
        there = part if there is None else there + part
    l_send[1] = there.astype(BF16)
    cross = remote(l_send.at[1], l_recv.at[core], l_ssem.at[1], l_rsem.at[1], (mate[0], other))
    cross.start()
    l_send[0] = here.astype(BF16)
    sends = [remote(l_send.at[0], l_recv.at[core], l_ssem.at[0], l_rsem.at[0], (a, other)), cross]
    sends[0].start()

    own_rows = pl.ds(pl.multiple_of(f * 256, 256), 256)
    mine = None
    for s in (0, 3, 1, 2):
        swaps[(0, 3, 1, 2).index(s)].wait_recv()
        if s:
            loans[4 - s, 0].wait_recv()
        both = jnp.concatenate([gat[0, s].reshape(256, 128), gat[1, s].reshape(256, 128)], axis=1)
        part = dot(lent[3 - s, 0] if s else ph[own_rows, :], both)
        mine = part if mine is None else mine + part
    l_own[...] = mine

    for c in answers:
        c.wait_recv()
    near = short[...] + sh_recv[0].astype(F32) + sh_recv[1].astype(F32)
    own = feats[own_rows, :].astype(F32)
    l_own[...] = l_own[...] + near * (1.0 / math.sqrt(TILE)) + own
    for c in sends:
        c.wait_recv()
    far = jnp.concatenate([l_recv[0].astype(F32), l_recv[1].astype(F32)], axis=1)
    out_ref[...] = (l_own[...] + far).astype(BF16)

    pltpu.make_async_copy(parts, parts, rs_ssem).wait()
    for s in range(4):
        left = rs_recv.at[pl.ds(1, 16 if s else 15)]
        pltpu.make_async_copy(left, left, ap_ssem.at[s]).wait()
    for c in asks + answers + shown + sends + swaps + list(loans.values()):
        c.wait_send()


def shards(feats, positions, phases, filt, w_value, neighbour_tiles, neighbour_count):
    n_atom = lax.axis_size("atom")
    n_freq = lax.axis_size("freq")
    scale = 1.0 / math.sqrt(feats.shape[0] * n_atom * phases.shape[2] * n_freq)
    in_hbm = pl.BlockSpec(memory_space=pltpu.HBM)
    vmem, dma = pltpu.VMEM, pltpu.SemaphoreType.DMA
    operands = [
        pltpu.with_memory_space_constraint(x, pltpu.HBM)
        for x in (feats, positions, phases, filt, w_value, neighbour_tiles, neighbour_count)
    ]
    return pl.pallas_call(
        functools.partial(kernel, scale),
        out_shape=jax.ShapeDtypeStruct((256, 256), BF16),
        in_specs=[in_hbm] * 7,
        out_specs=pl.BlockSpec(memory_space=pltpu.VMEM),
        scratch_shapes=[
            pltpu.SMEM((2, 8), jnp.int32),
            pltpu.SMEM((2,), jnp.int32),
            vmem((2048, 256), BF16),
            vmem((3, 2048), F32),
            vmem((2048, 256), BF16),
            vmem((3, 2, 256, 256), BF16),
            vmem((4, 256, 256), BF16),
            vmem((128, 256), F32),
            vmem((256, 256), BF16),
            vmem((2048, 256), BF16),
            vmem((256, 2048), BF16),
            vmem((8, 256), F32),
            vmem((16, 128), jnp.int32),
            vmem((2, 8, 256), F32),
            vmem((2, 16, 128), jnp.int32),
            vmem((3, 256, 128), F32),
            vmem((256, 256), F32),
            vmem((2, 256, 256), BF16),
            vmem((2, 256, 256), BF16),
            vmem((32, 16, 128), BF16),
            vmem((32, 16, 128), BF16),
            vmem((2, 4, 2, 8, 16, 128), BF16),
            vmem((256, 256), F32),
            vmem((2, 256, 128), BF16),
            vmem((2, 256, 128), BF16),
            dma((5 + 3 * CHUNKS,)),
            dma,
            dma,
            dma((6,)),
            dma((6,)),
            dma((4,)),
            dma((4,)),
            dma((4,)),
            dma((4,)),
            dma((2,)),
            dma((2,)),
            dma((4,)),
            dma((4,)),
            dma((4,)),
            dma((4,)),
            dma((2,)),
            dma((2,)),
        ],
        compiler_params=pltpu.CompilerParams(
            collective_id=0, has_side_effects=True, vmem_limit_bytes=40_000_000
        ),
    )(*operands)


def solution(mesh):
    in_specs = (
        P("atom", None),
        P(None, "atom"),
        P(None, "atom", "freq"),
        P("freq", None),
        P(),
        P(("atom", "freq"), None),
        P(("atom", "freq")),
    )
    out_specs = P(("atom", "freq"), None)
    return jax.shard_map(shards, mesh=mesh, in_specs=in_specs, out_specs=out_specs, check_vma=False)
```

```python
import functools
import math

import jax
import jax.numpy as jnp
from jax import lax
from jax.experimental import pallas as pl
from jax.experimental.pallas import tpu as pltpu
from jax.sharding import PartitionSpec as P

MESH = pl.DeviceIdType.MESH
TILE = 128
CHUNKS = 2
FAR = 1e30
LATE = ((2, 0),)
ATOM_PEERS = [(i, j, k) for i in (1, 0) for j in (4, 3, 5, 2, 6, 1, 7, 0) for k in (1, 0) if i + j + k > 0]

F32 = jnp.float32
BF16 = jnp.bfloat16


def dot(a, b):
    return jnp.dot(a, b, preferred_element_type=F32)


def kernel(
    scale,
    feats_hbm,
    pos_hbm,
    phases_hbm,
    filt_hbm,
    w_hbm,
    tiles_hbm,
    count_hbm,
    out_ref,
    tiles_smem,
    count_smem,
    feats,
    pos,
    ph,
    lent,
    seen,
    filt,
    w,
    values,
    weight,
    req_pos,
    req_ids,
    in_pos,
    in_ids,
    columns,
    short,
    sh_send,
    sh_recv,
    rs_send,
    rs_recv,
    gat,
    l_own,
    l_send,
    l_recv,
    in_sem,
    rs_ssem,
    rs_rsem,
    ph_ssem,
    ph_rsem,
    se_ssem,
    se_rsem,
    rq_ssem,
    rq_rsem,
    sh_ssem,
    sh_rsem,
    ap_ssem,
    ap_rsem,
    sw_ssem,
    sw_rsem,
    l_ssem,
    l_rsem,
):
    a = lax.axis_index("atom")
    f = lax.axis_index("freq")
    core = lax.rem(a, 2)
    row = a // 2
    x_lo = row // 8
    z = lax.rem(row, 8)
    x_hi = f // 4
    y = lax.rem(f, 4)
    other = (1 - x_hi) * 4 + y

    def remote(src, dst, ssem, rsem, to):
        return pltpu.make_async_remote_copy(
            src_ref=src, dst_ref=dst, send_sem=ssem, recv_sem=rsem, device_id=to, device_id_type=MESH
        )

    z_at = [lax.rem(z + j, 8) * 2 for j in range(8)]
    x_at = [x_lo * 16, (1 - x_lo) * 16]
    core_at = [core, 1 - core]

    def block_at(d):
        return x_at[d[0]] + z_at[d[1]] + core_at[d[2]]

    barrier = pltpu.get_barrier_semaphore()

    def greet(to):
        pl.semaphore_signal(barrier, inc=1, device_id=to, device_id_type=MESH)

    for d in ATOM_PEERS:
        greet((block_at(d), f))
    for j in (2, 1, 3):
        greet((a, x_hi * 4 + lax.rem(y + j, 4)))
    greet((a, other))

    step = 2048 // CHUNKS
    loads = [
        pltpu.make_async_copy(pos_hbm, pos, in_sem.at[0]),
        pltpu.make_async_copy(filt_hbm, filt, in_sem.at[1]),
        pltpu.make_async_copy(w_hbm, w, in_sem.at[2]),
        pltpu.make_async_copy(tiles_hbm, tiles_smem, in_sem.at[3]),
        pltpu.make_async_copy(count_hbm, count_smem, in_sem.at[4]),
    ]
    chunk_loads = []
    for i in range(CHUNKS):
        rows = pl.ds(i * step, step)
        trio = [
            pltpu.make_async_copy(phases_hbm.at[0, rows], ph.at[rows, pl.ds(0, 128)], in_sem.at[5 + 3 * i]),
            pltpu.make_async_copy(phases_hbm.at[1, rows], ph.at[rows, pl.ds(128, 128)], in_sem.at[6 + 3 * i]),
            pltpu.make_async_copy(feats_hbm.at[rows], feats.at[rows], in_sem.at[7 + 3 * i]),
        ]
        for c in trio:
            c.start()
        chunk_loads.append(trio)
    for c in loads:
        c.start()

    total = None
    for i in range(CHUNKS):
        for c in chunk_loads[i]:
            c.wait()
        rows = pl.ds(i * step, step)
        part = lax.dot_general(
            ph[rows, :], feats[rows, :], (((0,), (0,)), ((), ())), preferred_element_type=F32
        )
        total = part if total is None else total + part
    for h in range(2):
        rs_send[h * 16 : (h + 1) * 16] = total[:, h * 128 : (h + 1) * 128].astype(BF16).reshape(16, 16, 128)

    loads[0].wait()
    loads[3].wait()
    loads[4].wait()
    req_pos[...] = jnp.zeros_like(req_pos)
    req_pos[0:3, :] = pos[:, pl.ds(pl.multiple_of(f * 256, 256), 256)]
    for t in range(2):
        for n in range(8):
            tile = jnp.where(n < count_smem[t], tiles_smem[t, n], -1)
            req_ids[t * 8 + n : t * 8 + n + 1, :] = jnp.full((1, 128), tile, jnp.int32)

    pl.semaphore_wait(barrier, 35)

    for i, d in enumerate(ATOM_PEERS):
        to = block_at(d)
        share_of = core_at[d[2]] * 16 + (x_at[d[0]] + z_at[d[1]]) // 2
        remote(rs_send.at[share_of], rs_recv.at[i + 1], rs_ssem, rs_rsem, (to, f)).start()
    before, after = lax.rem(a + 31, 32), lax.rem(a + 1, 32)
    asks = []
    for i, to in enumerate((before, after)):
        asks.append(remote(req_pos, in_pos.at[i], rq_ssem.at[2 * i], rq_rsem.at[2 * i], (to, f)))
        asks.append(remote(req_ids, in_ids.at[i], rq_ssem.at[2 * i + 1], rq_rsem.at[2 * i + 1], (to, f)))
    for c in asks:
        c.start()

    def lend(j, hi):
        to = lax.rem(y + j, 4)
        rows = pl.ds(pl.multiple_of((lax.rem(x_hi + hi, 2) * 4 + to) * 256, 256), 256)
        i = (j - 1) * 2 + hi
        return remote(
            ph.at[rows], lent.at[j - 1, hi], ph_ssem.at[i], ph_rsem.at[i], (a, x_hi * 4 + to)
        )

    loans = {(j, hi): lend(j, hi) for hi in (1, 0) for j in (1, 3, 2)}
    for key in loans:
        if key not in LATE:
            loans[key].start()

    loads[2].wait()
    for i in range(CHUNKS):
        rows = pl.ds(i * step, step)
        values[rows, :] = dot(feats[rows, :], w[...]).astype(BF16)

    def query(pos_ref, ids_ref):
        flipped = pos_ref[...].T
        for c in range(3):
            columns[c] = jnp.broadcast_to(flipped[:, c : c + 1], (256, 128))

        def tile(s, carry):
            lanes = pl.ds(pl.multiple_of(s * TILE, TILE), TILE)
            mine = a * 16 + s
            theirs = pos[:, lanes]
            for t in range(2):
                rows = pl.ds(t * TILE, TILE)
                live = jnp.max((ids_ref[t * 8 : (t + 1) * 8, :] == mine).astype(F32), axis=0, keepdims=True)
                dist = (1.0 - live) * FAR
                for c in range(3):
                    diff = columns[c, rows, :] - theirs[c : c + 1, :]
                    dist = dist + diff * diff
                weight[rows, lanes] = jnp.exp(-dist).astype(BF16)
            return carry

        lax.fori_loop(0, 16, tile, 0)
        return dot(weight[...], values[...])

    short[...] = query(req_pos, req_ids)

    parts = rs_recv.at[pl.ds(1, 31)]
    pltpu.make_async_copy(parts, parts, rs_rsem).wait()
    share = rs_send[core * 16 + row].astype(F32)
    share = share + jnp.sum(rs_recv[1:32].astype(F32), axis=0)
    loads[1].wait()
    k_rows = pl.ds(pl.multiple_of(lax.rem(row, 8) * 16, 16), 16)
    filt_share = jnp.where(core == 0, filt[k_rows, 0:128], filt[k_rows, 128:256])
    gat[core, 0, x_lo, z] = (filt_share * share * scale).astype(BF16)

    y_at = [x_hi * 4 + lax.rem(y + j, 4) for j in range(4)]
    for j in (2, 1, 3, 0):
        for dz in (4, 3, 5, 2, 6, 1, 7, 0):
            for i in (1, 0):
                if dz + j + i > 0:
                    slot = (4 - j) % 4
                    remote(
                        gat.at[core, 0, x_lo, z],
                        gat.at[core, slot, x_lo, z],
                        ap_ssem.at[slot],
                        ap_rsem.at[slot],
                        (x_at[i] + z_at[dz] + core, y_at[j]),
                    ).start()

    for key in LATE:
        loans[key].start()

    answers = []

    def answer(i, to):
        asks[2 * i].wait_recv()
        asks[2 * i + 1].wait_recv()
        sh_send[i] = query(in_pos.at[i], in_ids.at[i]).astype(BF16)
        answers.append(remote(sh_send.at[i], sh_recv.at[i], sh_ssem.at[i], sh_rsem.at[i], (to, f)))

    answer(0, after)
    answers[0].start()
    answer(1, before)
    answers[1].start()

    twin_rows = pl.ds(pl.multiple_of(((1 - x_hi) * 4 + y) * 256, 256), 256)
    mate = (row * 2 + 1 - core, f)
    shown = [remote(ph.at[twin_rows], seen.at[0], se_ssem.at[0], se_rsem.at[0], mate)]
    shown[0].start()
    for j in (1, 3, 2):
        loans[j, 1].wait_recv()
        s = 4 - j
        shown.append(remote(lent.at[j - 1, 1], seen.at[s], se_ssem.at[s], se_rsem.at[s], mate))
        shown[-1].start()

    swaps = []
    here = there = None
    for i, s in enumerate((0, 3, 1, 2)):
        shown[i].wait_recv()
        arrived = rs_recv.at[pl.ds(1, 16 if s else 15)]
        pltpu.make_async_copy(arrived, arrived, ap_rsem.at[s]).wait()
        swaps.append(remote(gat.at[core, s], gat.at[core, s], sw_ssem.at[s], sw_rsem.at[s], mate))
        swaps[i].start()
        filtered = gat[core, s].reshape(256, 128)
        part = dot(lent[3 - s, 1] if s else ph[twin_rows, :], filtered)
        here = part if here is None else here + part
        part = dot(seen[s], filtered)
        there = part if there is None else there + part
    l_send[1] = there.astype(BF16)
    cross = remote(l_send.at[1], l_recv.at[core], l_ssem.at[1], l_rsem.at[1], (mate[0], other))
    cross.start()
    l_send[0] = here.astype(BF16)
    sends = [remote(l_send.at[0], l_recv.at[core], l_ssem.at[0], l_rsem.at[0], (a, other)), cross]
    sends[0].start()

    own_rows = pl.ds(pl.multiple_of(f * 256, 256), 256)
    mine = None
    for s in (0, 3, 1, 2):
        swaps[(0, 3, 1, 2).index(s)].wait_recv()
        if s:
            loans[4 - s, 0].wait_recv()
        both = jnp.concatenate([gat[0, s].reshape(256, 128), gat[1, s].reshape(256, 128)], axis=1)
        part = dot(lent[3 - s, 0] if s else ph[own_rows, :], both)
        mine = part if mine is None else mine + part
    l_own[...] = mine

    for c in answers:
        c.wait_recv()
    near = short[...] + sh_recv[0].astype(F32) + sh_recv[1].astype(F32)
    own = feats[own_rows, :].astype(F32)
    l_own[...] = l_own[...] + near * (1.0 / math.sqrt(TILE)) + own
    for c in sends:
        c.wait_recv()
    far = jnp.concatenate([l_recv[0].astype(F32), l_recv[1].astype(F32)], axis=1)
    out_ref[...] = (l_own[...] + far).astype(BF16)

    pltpu.make_async_copy(parts, parts, rs_ssem).wait()
    for s in range(4):
        left = rs_recv.at[pl.ds(1, 16 if s else 15)]
        pltpu.make_async_copy(left, left, ap_ssem.at[s]).wait()
    for c in asks + answers + shown + sends + swaps + list(loans.values()):
        c.wait_send()


def shards(feats, positions, phases, filt, w_value, neighbour_tiles, neighbour_count):
    n_atom = lax.axis_size("atom")
    n_freq = lax.axis_size("freq")
    scale = 1.0 / math.sqrt(feats.shape[0] * n_atom * phases.shape[2] * n_freq)
    in_hbm = pl.BlockSpec(memory_space=pltpu.HBM)
    vmem, dma = pltpu.VMEM, pltpu.SemaphoreType.DMA
    operands = [
        pltpu.with_memory_space_constraint(x, pltpu.HBM)
        for x in (feats, positions, phases, filt, w_value, neighbour_tiles, neighbour_count)
    ]
    return pl.pallas_call(
        functools.partial(kernel, scale),
        out_shape=jax.ShapeDtypeStruct((256, 256), BF16),
        in_specs=[in_hbm] * 7,
        out_specs=pl.BlockSpec(memory_space=pltpu.VMEM),
        scratch_shapes=[
            pltpu.SMEM((2, 8), jnp.int32),
            pltpu.SMEM((2,), jnp.int32),
            vmem((2048, 256), BF16),
            vmem((3, 2048), F32),
            vmem((2048, 256), BF16),
            vmem((3, 2, 256, 256), BF16),
            vmem((4, 256, 256), BF16),
            vmem((128, 256), F32),
            vmem((256, 256), BF16),
            vmem((2048, 256), BF16),
            vmem((256, 2048), BF16),
            vmem((8, 256), F32),
            vmem((16, 128), jnp.int32),
            vmem((2, 8, 256), F32),
            vmem((2, 16, 128), jnp.int32),
            vmem((3, 256, 128), F32),
            vmem((256, 256), F32),
            vmem((2, 256, 256), BF16),
            vmem((2, 256, 256), BF16),
            vmem((32, 16, 128), BF16),
            vmem((32, 16, 128), BF16),
            vmem((2, 4, 2, 8, 16, 128), BF16),
            vmem((256, 256), F32),
            vmem((2, 256, 128), BF16),
            vmem((2, 256, 128), BF16),
            dma((5 + 3 * CHUNKS,)),
            dma,
            dma,
            dma((6,)),
            dma((6,)),
            dma((4,)),
            dma((4,)),
            dma((4,)),
            dma((4,)),
            dma((2,)),
            dma((2,)),
            dma((4,)),
            dma((4,)),
            dma((4,)),
            dma((4,)),
            dma((2,)),
            dma((2,)),
        ],
        compiler_params=pltpu.CompilerParams(
            collective_id=0, has_side_effects=True, vmem_limit_bytes=40_000_000
        ),
    )(*operands)


def solution(mesh):
    in_specs = (
        P("atom", None),
        P(None, "atom"),
        P(None, "atom", "freq"),
        P("freq", None),
        P(),
        P(("atom", "freq"), None),
        P(("atom", "freq")),
    )
    out_specs = P(("atom", "freq"), None)
    return jax.shard_map(shards, mesh=mesh, in_specs=in_specs, out_specs=out_specs, check_vma=False)
```
